256 devices in a mesh: rep: 1, dp: 256 (over x, y, z, core).
Axes of the slice: x: 4, y: 4, z: 8, core: 2. Of those that a mesh axis runs over, the one named last changes fastest.
Arguments:
- g_w_gate: bfloat16 [256, 2, 768, 2048], P(('rep', 'dp'))
- g_w_up: bfloat16 [256, 2, 768, 2048], P(('rep', 'dp'))
- g_w_down: bfloat16 [256, 2, 2048, 768], P(('rep', 'dp'))
- w_gate: bfloat16 [2, 768, 2048], replicated
- w_up: bfloat16 [2, 768, 2048], replicated
- w_down: bfloat16 [2, 2048, 768], replicated
- m_w_gate: float32 [2, 768, 2048], P(None, 'dp')
- m_w_up: float32 [2, 768, 2048], P(None, 'dp')
- m_w_down: float32 [2, 2048, 768], P(None, 'dp')
- v_w_gate: float32 [2, 768, 2048], P(None, 'dp')
- v_w_up: float32 [2, 768, 2048], P(None, 'dp')
- v_w_down: float32 [2, 2048, 768], P(None, 'dp')
Outputs:
- output 1: bfloat16 [2, 768, 2048], P('rep')
- output 2: bfloat16 [2, 768, 2048], P('rep')
- output 3: bfloat16 [2, 2048, 768], P('rep')
- output 4: float32 [2, 768, 2048], P('rep', 'dp')
- output 5: float32 [2, 768, 2048], P('rep', 'dp')
- output 6: float32 [2, 2048, 768], P('rep', 'dp')
- output 7: float32 [2, 768, 2048], P('rep', 'dp')
- output 8: float32 [2, 768, 2048], P('rep', 'dp')
- output 9: float32 [2, 2048, 768], P('rep', 'dp')
All inputs are finite; a program needn't handle non-finite values.
Results may differ from the reference program's by a relative error of at most 0.022.
Values are sent between devices in bfloat16 or wider.
A program may use at most 768 MiB of HBM per device.

```python
import jax
import jax.numpy as jnp
from jax import lax

DEVICES = 256
D = 768
FF = 2048
LAYERS = 2
NAMES = ("w_gate", "w_up", "w_down")
SHAPES = {"w_gate": (LAYERS, D, FF), "w_up": (LAYERS, D, FF), "w_down": (LAYERS, FF, D)}


def setup_inputs(seed: int = 0, part: int = 0) -> dict:
    kz, *keys = jax.random.split(jax.random.key(seed), 1 + 5 * len(NAMES))
    loud = 2.0 ** jax.random.uniform(kz, (), jnp.float32, -1.0, 1.0)
    drawn = {}
    for name, key, both in zip(NAMES, keys[:3], keys[3:6], strict=True):
        own = jax.random.normal(jax.random.fold_in(key, part), (DEVICES, *SHAPES[name]), jnp.float32)
        shared = jax.random.normal(jax.random.fold_in(both, part), SHAPES[name], jnp.float32)
        drawn["g_" + name] = (loud * (0.7 * shared / DEVICES + 0.7 * own * DEVICES**-0.5)).astype(jnp.bfloat16)
    for name, key in zip(NAMES, keys[6:9], strict=True):
        drawn[name] = (jax.random.normal(key, SHAPES[name], jnp.float32) * SHAPES[name][1] ** -0.5).astype(jnp.bfloat16)
    for name, key in zip(NAMES, keys[9:12], strict=True):
        drawn["m_" + name] = loud * 0.5 * jax.random.normal(key, SHAPES[name], jnp.float32)
    for name, key in zip(NAMES, keys[12:15], strict=True):
        drawn["v_" + name] = loud * loud * jax.random.uniform(key, SHAPES[name], jnp.float32, 0.5, 1.5)
    return drawn


def adamw(w, m, v, g):
    m = 0.9 * m + 0.1 * g
    v = 0.95 * v + 0.05 * g * g
    step = m * lax.rsqrt(v + 1e-8) + 0.1 * w
    return (w - 0.02 * step).astype(jnp.bfloat16), m, v


def clipped(gradients, sum_of_squares, count):
    factor = jnp.minimum(1.0, 0.5 * lax.rsqrt(sum_of_squares / count + 1e-30))
    return [g * factor for g in gradients]


def reference(g_w_gate, g_w_up, g_w_down, w_gate, w_up, w_down, m_w_gate, m_w_up, m_w_down, v_w_gate, v_w_up, v_w_down):
    def total(terms):
        return lax.scan(lambda so_far, term: (so_far + term.astype(jnp.float32), None), jnp.zeros(terms.shape[1:], jnp.float32), terms)[0]

    gradients = [total(terms).astype(jnp.bfloat16).astype(jnp.float32) for terms in (g_w_gate, g_w_up, g_w_down)]
    gradients = clipped(gradients, sum(jnp.sum(g * g) for g in gradients), sum(g.size for g in gradients))
    new = [
        adamw(w.astype(jnp.float32), m, v, g)
        for w, m, v, g in zip((w_gate, w_up, w_down), (m_w_gate, m_w_up, m_w_down), (v_w_gate, v_w_up, v_w_down), gradients, strict=True)
    ]
    return tuple(one[which] for which in range(3) for one in new)
```

```python
import math

import jax
import jax.numpy as jnp
from jax import lax
from jax.experimental import pallas as pl
from jax.experimental.pallas import tpu as pltpu
from jax.sharding import PartitionSpec as P

N, NZ, COLUMN = 4, 8, 16
LAYERS, ROWS, LANES = 2, 16, 128
TILES, WIDE, NARROW = 3, 1024, 384
SLAB = 8
F32, BF16 = jnp.float32, jnp.bfloat16
MESH = pl.DeviceIdType.MESH
BIG, SMALL = (0, 2), (2, 1)
SEMAPHORES = 201
VMEM_LIMIT = 36 * 2**20


def add_refs(dst, srcs, dims):
    @pl.loop(0, math.prod(dims))
    def _(i):
        at = []
        for d in reversed(dims):
            at.insert(0, i % d)
            i = i // d
        at = tuple(at)
        total = srcs[0][at].astype(F32)
        for s in srcs[1:]:
            total = total + s[at].astype(F32)
        dst[at] = total.astype(dst.dtype)


def order(n):
    half, seq = n // 2, []
    for s in range(1, half + 1):
        seq.append((True, s))
        if s < half:
            seq.append((False, s))
    return seq


def interleave(*some):
    live = [[next(r), r] for r in some]
    while live:
        first = min(live, key=lambda o: o[0])
        yield first[0]
        first[0] = next(first[1], None)
        if first[0] is None:
            live.remove(first)


def chain(*some):
    for one in some:
        yield from one


def run(generator):
    for _ in generator:
        pass


def tiles(part):
    return pl.ds(part[0], part[1])


def adamw(w, m, v, g):
    m = 0.9 * m + 0.1 * g
    v = 0.95 * v + 0.05 * g * g
    step = m * lax.rsqrt(v + 1e-8) + 0.1 * w
    return (w - 0.02 * step).astype(BF16), m, v


def kernel(
    gG, gU, gD, wG, wU, wD, mG, mU, mD, vG, vU, vD, oG, oU, oD, back, backD,
    ownG, peerG, ownU, peerU, ownD, peerD, accG, accU, accD, accZ, accY,
    r1G, r1U, r1D, r2G, s2G, r2U, s2U, r2D, s2D, rY, sY, rZ, sZ,
    gsum, gsumD, wcol, wcolD, mvcol, mvD, pk, pkr, pk2, nrm, nr1, nr2, sems,
):
    me = lax.axis_index("dp")
    c, k, xy = me % 2, me % COLUMN, me // COLUMN
    z, y, x = k // 2, xy % N, xy // N
    cb = c * NZ + z

    def dev(x, y, z, c):
        return {"dp": ((x * N + y) * NZ + z) * 2 + c}

    def in_column(kk):
        return {"dp": xy * COLUMN + kk}

    partner = dev(x, y, z, 1 - c)
    ring_ids = {
        "x": (dev((x + 1) % N, y, z, c), dev((x + N - 1) % N, y, z, c)),
        "y": (dev(x, (y + 1) % N, z, c), dev(x, (y + N - 1) % N, z, c)),
        "z": (dev(x, y, (z + 1) % NZ, c), dev(x, y, (z + NZ - 1) % NZ, c)),
    }
    used = []

    def sem():
        used.append(None)
        return sems.at[len(used) - 1]

    def remote(src, dst, ssem, rsem, device):
        return pltpu.make_async_remote_copy(src_ref=src, dst_ref=dst, send_sem=ssem, recv_sem=rsem, device_id=device, device_id_type=MESH)

    sent = []

    def group(ref):
        one = sem()
        sent.append((one, ref))
        return one

    def wait_all(one, ref):
        remote(ref, ref, one, one, partner).wait_recv()

    barrier = pltpu.get_barrier_semaphore()
    for j in range(1, COLUMN):
        pl.semaphore_signal(barrier, inc=1, device_id=in_column((k + j) % COLUMN), device_id_type=MESH)
        pl.semaphore_signal(barrier, inc=1, device_id={"dp": (xy + j) % COLUMN * COLUMN + k}, device_id_type=MESH)

    def wide(c):
        return pl.ds(pl.multiple_of(c * WIDE, WIDE), WIDE)

    def narrow(c):
        return pl.ds(pl.multiple_of(c * NARROW, NARROW), NARROW)

    def slab(c):
        return pl.ds(pl.multiple_of(c * SLAB, SLAB), SLAB)

    def block(mat, b, c):
        if mat == "G":
            return gG.at[:, b, :, :, :, wide(c)]
        if mat == "U":
            return gU.at[:, :, b, :, :, wide(c)]
        return gD.at[:, :, :, b, :, narrow(c)]

    own = {"G": ownG, "U": ownU, "D": ownD}
    peer = {"G": peerG, "U": peerU, "D": peerD}
    first = {"G": (x, N), "U": (y, N), "D": (z, NZ)}
    acc = {"G": accG, "U": accU, "D": accD}
    r1 = {"G": r1G, "U": r1U, "D": r1D}
    r2 = {"G": r2G, "U": r2U, "D": r2D}
    s2 = {"G": s2G, "U": s2U, "D": s2D}
    need = [("D", 4), ("G", 2), ("U", 2), ("D", 3), ("D", -3), ("D", 2), ("D", -2), ("G", 1), ("G", -1),
            ("U", 1), ("U", -1), ("D", 1), ("D", -1), ("G", 0), ("U", 0), ("D", 0)]

    def at(mat, off):
        p, n = first[mat]
        return (p + off + n) % n

    loaded = {mat: sem() for mat in own}
    for mat, off in need:
        b = at(mat, off)
        pltpu.make_async_copy(block(mat, b, c), own[mat].at[b], loaded[mat]).start()
    mine = pl.ds(pl.multiple_of(cb * LANES, LANES), LANES)
    wloads = [pltpu.make_async_copy(w.at[:, x, y, :, :, mine], wcol.at[i], sem()) for i, w in enumerate((wG, wU))]
    wloads.append(pltpu.make_async_copy(wD.at[:, x, y, z, :, narrow(c)], wcolD, sem()))
    for one in wloads:
        one.start()

    for j, ref in enumerate((mG, vG, mU, vU)):
        for l in range(LAYERS):
            for q in range(COLUMN):
                pk[q, j, TILES * l : TILES * l + TILES, :] = ref[:, l, LANES * q : LANES * q + LANES]
    for j, ref in enumerate((mD, vD)):
        mvD[j, :, slab(c), :] = ref[:, :, narrow(c)]

    with jax.named_scope("barrier"):
        pl.semaphore_wait(barrier, 2 * COLUMN - 2)

    peers, by_mat = {}, {mat: group(own[mat]) for mat in own}
    for mat, off in need:
        b = at(mat, off)
        peers[mat, off] = remote(block(mat, b, 1 - c), peer[mat].at[b], by_mat[mat], sem(), partner)
        peers[mat, off].start()

    landed = set()

    def local1(mat, off, b, half):
        if mat not in landed:
            landed.add(mat)
            pltpu.make_async_copy(own[mat], own[mat], loaded[mat]).wait()
        if (mat, off) not in landed:
            landed.add((mat, off))
            peers[mat, off].wait_recv()
        return [own[mat].at[b, half], peer[mat].at[b, half]]

    def rs_ring(name, axis, n, pos, local, send, recv, cut, ssem, dims, finish, times):
        seq, copies = order(n), {}
        for i, (far, s) in enumerate(seq):
            prev = seq.index((far, s - 1)) if s > 1 else None
            yield times[i]
            with jax.named_scope(f"{name}_{i}"):
                for d in range(2):
                    half = d if far else 1 - d
                    off = n // 2 - s + far
                    off = -off if d and off < n // 2 else off
                    b = (pos + off + n) % n
                    srcs = [cut(r) for r in local(off, b, half)]
                    if s > 1:
                        copies[d, prev].wait_recv()
                        srcs.append(cut(recv.at[d, prev]))
                    dst = cut(send(d, i, b, half))
                    add_refs(dst, srcs, dims)
                    copies[d, i] = remote(dst, cut(recv.at[d, i]), ssem, sem(), ring_ids[axis][d])
                    copies[d, i].start()
        yield times[-1]
        with jax.named_scope(f"{name}_end"):
            for half in range(2):
                copies[half, n - 2].wait_recv()
                copies[1 - half, n - 3].wait_recv()
                finish(half, [cut(recv.at[half, n - 2]), cut(recv.at[1 - half, n - 3])])

    def stage1(mat, axis, cut, ssem, dims, times):
        p, n = first[mat]

        def finish(half, got):
            add_refs(cut(acc[mat].at[half]), [cut(r) for r in local1(mat, 0, p, half)] + got, dims)

        return rs_ring(
            "rs" + mat + axis, axis, n, p, lambda off, b, half: local1(mat, off, b, half), lambda d, i, b, half: own[mat].at[b, half],
            r1[mat], cut, ssem, dims, finish, times,
        )

    def stage2(mat, axis, pos, cut, ssem, dims, finish, times):
        return rs_ring(
            "rs" + mat + axis, axis, N, pos, lambda off, b, half: [acc[mat].at[half, b]], lambda d, i, b, half: s2[mat].at[d, i],
            r2[mat], cut, ssem, dims, finish, times,
        )

    def to_z(which, mat, pos, part):
        def finish(half, got):
            here = acc[mat].at[half, pos, tiles(part)]

            @pl.loop(0, part[1])
            def _(i):
                total = here[i] + got[0][i].astype(F32) + got[1][i].astype(F32)
                for q in range(NZ):
                    one = total[:, LANES * q : LANES * q + LANES]
                    accZ[q, half, which, part[0] + i] = one
                    sZ[q, half, which, part[0] + i] = one.astype(BF16)

        return finish

    ss = {key: group(r) for key, r in (("G1", r1G), ("U1", r1U), ("D1", r1D), ("G2", r2G), ("U2", r2U), ("D2", r2D))}
    ss["Z"], ss["Y"] = group(rZ.at[: NZ - 1]), group(rY.at[: N - 1])

    def across_z(part, times):
        got, cut = sem(), tiles(part)
        yield times[0]
        for j in range(1, NZ):
            zz = (z + j) % NZ
            remote(sZ.at[zz, :, :, cut], rZ.at[z, :, :, cut], ss["Z"], got, dev(x, y, zz, c)).start()
        yield times[1]
        with jax.named_scope("rsZ"):
            wait_all(got, rZ.at[: NZ - 1, :, :, cut])

            @pl.loop(0, 2 * LAYERS)
            def _(i):
                half, which = i // 2, i % 2
                for t in range(part[0], sum(part)):
                    total = accZ[z, half, which, t]
                    for j in range(1, NZ):
                        total = total + rZ[(z + j) % NZ, half, which, t].astype(F32)
                    gsum[half, which, t] = total.astype(BF16).astype(F32)

    def rs_pipe(part, t1, t2, tz):
        cut1, cut2, n = (lambda r: r.at[:, tiles(part)]), (lambda r: r.at[tiles(part)]), part[1]
        return chain(
            interleave(
                chain(stage1("G", "x", cut1, ss["G1"], (N, n), t1), stage2("G", "y", y, cut2, ss["G2"], (n,), to_z(0, "G", y, part), t2)),
                chain(stage1("U", "y", cut1, ss["U1"], (N, n), t1), stage2("U", "x", x, cut2, ss["U2"], (n,), to_z(1, "U", x, part), t2)),
            ),
            across_z(part, tz),
        )

    def finishDx(half, got):
        @pl.loop(0, N)
        def _(i):
            total = accD[half, x, i] + got[0][i].astype(F32) + got[1][i].astype(F32)
            accY[half, i] = total
            sY[i, half] = total.astype(BF16)

    def across_y(times):
        got = sem()
        yield times[0]
        for j in range(1, N):
            yy = (y + j) % N
            remote(sY.at[yy], rY.at[y], ss["Y"], got, dev(x, yy, z, c)).start()
        yield times[1]
        with jax.named_scope("rsY"):
            wait_all(got, rY.at[: N - 1])
            for half in range(LAYERS):
                total = accY[half, y]
                for j in range(1, N):
                    total = total + rY[(y + j) % N, half].astype(F32)
                gsumD[half] = total.astype(BF16).astype(F32)

    whole = lambda r: r
    mv, mvd = sem(), sem()

    def send_moments():
        yield 31.0
        ssem, ssemD = group(pk.at[: COLUMN - 1]), group(mvD.at[:, :, :SLAB])
        for j in range(1, COLUMN):
            kk = (k + j) % COLUMN
            remote(pk.at[(kk % 2) * NZ + kk // 2], pkr.at[k], ssem, mv, in_column(kk)).start()
        for j, ref in enumerate((mD, vD)):
            remote(ref.at[:, :, narrow(1 - c)], mvD.at[j, :, slab(c)], ssemD, mvd, partner).start()

    run(interleave(
        chain(
            stage1("D", "z", whole, ss["D1"], (N, N), (-1.0, 0.7, 6.7, 10.9, 15.1, 19.3, 23.5, 32.0)),
            stage2("D", "x", x, whole, ss["D2"], (N,), finishDx, (32.0, 32.0, 36.2, 39.5)),
            across_y((39.5, 43.0)),
        ),
        rs_pipe(BIG, (0.0, 1.0, 8.5, 22.6), (22.6, 22.6, 29.0, 33.0), (33.0, 42.0)),
        rs_pipe(SMALL, (5.0, 12.0, 16.7, 28.2), (28.2, 28.2, 33.5, 36.5), (36.5, 44.0)),
        send_moments(),
    ))

    with jax.named_scope("norm"):
        total = jnp.zeros((SLAB, LANES), F32)

        def squares(total, g):
            for q in range(g.shape[1] // LANES):
                one = g[:, LANES * q : LANES * q + LANES]
                one = one * one
                total = total + one[:SLAB] + one[SLAB:]
            return total

        for half in range(LAYERS):
            for which in range(2):
                for t in range(TILES):
                    total = squares(total, gsum[half, which, t])
            total = squares(total, gsumD[half])
    for stage, got in enumerate((nr1, nr2)):
        with jax.named_scope(f"norm{stage}"):
            nrm[stage] = total
            here, rsem, ssem = (xy if stage else k), sem(), group(got.at[: COLUMN - 1])
            for j in range(1, COLUMN):
                there = (here + j) % COLUMN
                device = {"dp": there * COLUMN + k} if stage else in_column(there)
                remote(nrm.at[stage], got.at[here], ssem, rsem, device).start()
            if not stage:
                pkr[k] = pk[cb]
                wait_all(mv, pkr.at[: COLUMN - 1])
                for j in range(mvcol.shape[0]):
                    for l in range(LAYERS):
                        for q in range(COLUMN):
                            mvcol[j, l, TILES * q : TILES * q + TILES, :] = pkr[q, j, TILES * l : TILES * l + TILES, :]
                wait_all(mvd, mvD.at[:, :, :SLAB])
                for one in wloads:
                    one.wait()
            got[here] = nrm[stage]
            wait_all(rsem, got.at[: COLUMN - 1])
            total = got[0]
            for j in range(1, COLUMN):
                total = total + got[j]
    total = jnp.sum(jnp.sum(total, axis=1, keepdims=True), axis=0, keepdims=True)
    factor = jnp.minimum(1.0, 0.5 * lax.rsqrt(total / (3 * 2 * 768 * 2048) + 1e-30))

    with jax.named_scope("adamw"):
        for half in range(LAYERS):
            new, m, v = adamw(wcolD[half].astype(F32), mvD[0, half], mvD[1, half], gsumD[half] * factor)
            oD[half, x, y, z, :, narrow(c)] = new
            mvD[0, half] = m
            mvD[1, half] = v
            for a, out in enumerate((oG, oU)):
                for b in range(TILES):
                    rows, at_m, at_v = pl.ds(ROWS * b, ROWS), 2 * a, 2 * a + 1
                    new, m, v = adamw(
                        wcol[a, half, b].astype(F32), mvcol[at_m, half, rows], mvcol[at_v, half, rows], gsum[half, a, b] * factor
                    )
                    out[half, x, y, b, :, mine] = new
                    mvcol[at_m, half, rows] = m
                    mvcol[at_v, half, rows] = v

    onward = {mat: (group(peer[mat]), sem()) for mat in peer}

    def ag_ring(name, axis, n, pos, piece, ssem, on, times):
        seq, copies = order(n), {}

        def pass_on(ref):
            if on:
                remote(ref, ref, *onward[on], partner).start()

        def got(d, i):
            far, s = seq[i]
            copies[d, i].wait_recv()
            pass_on(piece((pos + (s if d else n - s)) % n, d if far else 1 - d))

        for i, (far, s) in enumerate(seq):
            yield times[i]
            with jax.named_scope(f"{name}_{i}"):
                for d in range(2):
                    if s > 1:
                        got(d, seq.index((far, s - 1)))
                    ref = piece((pos + (s - 1 if d else n - s + 1)) % n, d if far else 1 - d)
                    copies[d, i] = remote(ref, ref, ssem, sem(), ring_ids[axis][d])
                    copies[d, i].start()
        for half in range(2):
            pass_on(piece(pos, half))
        for slot in (n - 3, n - 2):
            yield times[slot + 2]
            with jax.named_scope(f"{name}_end{slot}"):
                for d in range(2):
                    got(d, slot)

    ss = {key: group(r) for key, r in (("G1", r1G), ("U1", r1U), ("D1", r1D), ("G2", r2G), ("U2", r2U), ("D2", r2D))}
    ss["Z"], ss["Y"] = group(rZ.at[: NZ - 1]), group(rY.at[: N - 1])

    def back_z(part, times):
        got = sem()
        yield times[0]
        for j in range(1, NZ):
            for out in (oG, oU):
                ref = out.at[:, x, y, tiles(part), :, mine]
                remote(ref, ref, ss["Z"], got, dev(x, y, (z + j) % NZ, c)).start()
        yield times[1]
        with jax.named_scope("agZ"):
            wait_all(got, rZ.at[: NZ - 1, :, :, tiles(part)])

    def back_y(times):
        got = sem()
        yield times[0]
        ref = oD.at[:, x, y, z, :, narrow(c)]
        for j in range(1, N):
            remote(ref, ref, ss["Y"], got, dev(x, (y + j) % N, z, c)).start()
        yield times[1]
        with jax.named_scope("agY"):
            wait_all(got, rY.at[: N - 1])

    def ag_pipe(part, tz, t2, t1):
        cols, cut = wide(c), tiles(part)
        return chain(
            back_z(part, tz),
            interleave(
                chain(
                    ag_ring("agGy", "y", N, y, lambda p, half: oG.at[half, x, p, cut, :, cols], ss["G2"], None, t2),
                    ag_ring("agGx", "x", N, x, lambda p, half: oG.at[half, p, :, cut, :, cols], ss["G1"], "G", t1),
                ),
                chain(
                    ag_ring("agUx", "x", N, x, lambda p, half: oU.at[half, p, y, cut, :, cols], ss["U2"], None, t2),
                    ag_ring("agUy", "y", N, y, lambda p, half: oU.at[half, :, p, cut, :, cols], ss["U1"], "U", t1),
                ),
            ),
        )

    rb, rd = sem(), sem()

    def return_moments():
        yield 14.0
        for q in range(COLUMN):
            for j in range(mvcol.shape[0]):
                for l in range(LAYERS):
                    pk2[q, j, TILES * l : TILES * l + TILES, :] = mvcol[j, l, TILES * q : TILES * q + TILES, :]
        ssem, ssemD = group(pk2.at[: COLUMN - 1]), group(backD.at[:, 0])
        for j in range(1, COLUMN):
            kk = (k + j) % COLUMN
            remote(pk2.at[kk], back.at[cb], ssem, rb, in_column(kk)).start()
        for j in range(2):
            remote(mvD.at[j, :, slab(1 - c)], backD.at[j, c], ssemD, rd, partner).start()
            backD[j, c] = mvD[j, :, slab(c)]
        back[cb] = pk2[k]

    run(interleave(
        chain(
            back_y((0.0, 4.0)),
            ag_ring("agDx", "x", N, x, lambda p, half: oD.at[half, p, :, z, :, narrow(c)], ss["D2"], None, (4.0, 4.0, 7.8, 9.2, 10.5)),
            ag_ring("agDz", "z", NZ, z, lambda p, half: oD.at[half, :, :, p, :, narrow(c)], ss["D1"], "D",
                    (10.5, 10.5, 17.3, 21.5, 25.7, 29.9, 34.1, 38.3, 42.5)),
        ),
        ag_pipe(SMALL, (0.1, 7.5), (7.5, 7.5, 10.9, 12.0, 12.6), (12.6, 12.6, 18.0, 21.0, 23.5)),
        ag_pipe(BIG, (0.2, 13.0), (13.0, 13.0, 17.2, 18.6, 20.0), (20.0, 20.0, 29.0, 35.0, 40.5)),
        return_moments(),
    ))

    with jax.named_scope("drain"):
        wait_all(rb, back.at[: COLUMN - 1])
        wait_all(rd, backD.at[:, 0])
        for mat in peer:
            wait_all(onward[mat][1], peer[mat])
        for one, ref in sent:
            remote(ref, ref, one, one, partner).wait_send()
    assert len(used) == SEMAPHORES, len(used)


def store(iG, iU, iD, packed, packedD, oG, oU, oD, omG, omU, omD, ovG, ovU, ovD, sem):
    pairs = ((iG, oG), (iU, oU), (iD, oD))
    for j, (i, o) in enumerate(pairs):
        for l in range(LAYERS):
            for p in range(N):
                pltpu.make_async_copy(i.at[l, p], o.at[l, p], sem.at[j]).start()
    for j, out in enumerate((omG, ovG, omU, ovU)):
        for l in range(LAYERS):
            for q in range(COLUMN):
                out[:, l, LANES * q : LANES * q + LANES] = packed[q, j, TILES * l : TILES * l + TILES, :]
    for j, out in enumerate((omD, ovD)):
        for h in range(2):
            out[:, :, NARROW * h : NARROW * h + NARROW] = packedD[j, h]
    for j, (i, o) in enumerate(pairs):
        pltpu.make_async_copy(i, o, sem.at[j]).wait()


def fused(*arrays):
    g, w, m, v = (arrays[i : i + 3] for i in (0, 3, 6, 9))
    big, low = (N, TILES, ROWS, WIDE), (N, N, ROWS, NARROW)
    view = (LAYERS, N, N, TILES, ROWS, 2 * WIDE)
    views = [view, view, (LAYERS, N, N, NZ, ROWS, 2 * NARROW)]
    g = [one.reshape(s) for one, s in zip(g, views, strict=True)]
    w = [one.reshape(s) for one, s in zip(w, views, strict=True)]
    m, v = ([jnp.swapaxes(one, 0, 1) if one.shape[1] == TILES else one for one in t] for t in (m, v))
    vm, hbm, D = pl.BlockSpec(memory_space=pltpu.VMEM), pl.BlockSpec(memory_space=pl.ANY), pltpu.SemaphoreType.DMA

    def V(dtype, *shape):
        return pltpu.VMEM(shape, dtype)

    tile, packed, packedD = (TILES, ROWS, LANES), (COLUMN, N, SLAB, LANES), (2, 2, LAYERS, SLAB, NARROW)
    scratch = [
        *[V(BF16, N, LAYERS, *big)] * 4, *[V(BF16, NZ, LAYERS, *low)] * 2,
        *[V(F32, LAYERS, *big)] * 2, V(F32, LAYERS, *low), V(F32, NZ, LAYERS, 2, *tile), V(F32, LAYERS, *low[1:]),
        *[V(BF16, 2, N - 1, *big)] * 2, V(BF16, 2, NZ - 1, *low),
        *[V(BF16, 2, N - 1, *big[1:])] * 4, *[V(BF16, 2, N - 1, *low[1:])] * 2,
        *[V(BF16, N, LAYERS, *low[2:])] * 2, *[V(BF16, NZ, LAYERS, 2, *tile)] * 2,
        V(F32, LAYERS, 2, *tile), V(F32, LAYERS, *low[2:]), V(BF16, 2, LAYERS, *tile), V(BF16, LAYERS, *low[2:]),
        V(F32, N, LAYERS, TILES * ROWS, LANES), V(F32, 2, LAYERS, *low[2:]), *[V(F32, *packed)] * 3,
        V(F32, 2, SLAB, LANES), *[V(F32, COLUMN, SLAB, LANES)] * 2, D((SEMAPHORES,)),
    ]
    passed = pl.pallas_call(
        kernel,
        out_shape=[V(BF16, *s) for s in views] + [V(F32, *packed), V(F32, *packedD)],
        in_specs=[hbm] * 6 + [vm] * 6,
        out_specs=[vm] * 5,
        scratch_shapes=scratch,
        compiler_params=pltpu.CompilerParams(collective_id=0, has_side_effects=True, vmem_limit_bytes=VMEM_LIMIT),
        name="step",
    )(*g, *w, *m, *v)
    outs = pl.pallas_call(
        store,
        out_shape=[jax.ShapeDtypeStruct(s, BF16) for s in views] + [jax.ShapeDtypeStruct(one.shape, F32) for one in (*m, *v)],
        in_specs=[vm] * 5,
        out_specs=[hbm] * 3 + [vm] * 6,
        scratch_shapes=[D((3,))],
        compiler_params=pltpu.CompilerParams(vmem_limit_bytes=2**20),
        name="store",
    )(*passed)
    outs = [jnp.swapaxes(o, 0, 1) if o.shape[0] == TILES else o for o in outs]
    return tuple(o.reshape(one.shape) for o, one in zip(outs, (*arrays[3:6], *arrays[6:]), strict=True))


def solution(mesh):
    all_of, cut = P(None, None, None), P(None, "dp", None)
    return jax.shard_map(
        fused,
        mesh=mesh,
        in_specs=(P(("rep", "dp"), None, None, None),) * 3 + (all_of,) * 3 + (cut,) * 6,
        out_specs=(P("rep", None, None),) * 3 + (P("rep", "dp", None),) * 6,
        check_vma=False,
    )
```

```python
import math

import jax
import jax.numpy as jnp
from jax import lax
from jax.experimental import pallas as pl
from jax.experimental.pallas import tpu as pltpu
from jax.sharding import PartitionSpec as P

N, NZ, COLUMN = 4, 8, 16
LAYERS, ROWS, LANES = 2, 16, 128
TILES, WIDE, NARROW = 3, 1024, 384
SLAB = 8
F32, BF16 = jnp.float32, jnp.bfloat16
MESH = pl.DeviceIdType.MESH
KEPT, REUSED = 11, 150
VMEM_LIMIT = 36 * 2**20


def add_refs(dst, srcs, dims):
    @pl.loop(0, math.prod(dims))
    def _(i):
        at = []
        for d in reversed(dims):
            at.insert(0, i % d)
            i = i // d
        at = tuple(at)
        total = srcs[0][at].astype(F32)
        for s in srcs[1:]:
            total = total + s[at].astype(F32)
        dst[at] = total.astype(dst.dtype)


def order(n):
    half, seq = n // 2, []
    for s in range(1, half + 1):
        seq.append((True, s))
        if s < half:
            seq.append((False, s))
    return seq


def interleave(*some):
    live = [[next(r), r] for r in some]
    while live:
        first = min(live, key=lambda o: o[0])
        yield first[0]
        first[0] = next(first[1], None)
        if first[0] is None:
            live.remove(first)


def chain(*some):
    for one in some:
        yield from one


def run(generator):
    for _ in generator:
        pass


def tiles(part):
    return pl.ds(part, 1)


def adamw(w, m, v, g):
    m = 0.9 * m + 0.1 * g
    v = 0.95 * v + 0.05 * g * g
    step = m * lax.rsqrt(v + 1e-8) + 0.1 * w
    return (w - 0.02 * step).astype(BF16), m, v


def kernel(
    gG, gU, gD, wG, wU, wD, hmG, hmU, hmD, hvG, hvU, hvD, oG, oU, oD, back, backD,
    ownG, peerG, ownU, peerU, ownD, peerD, accG, accU, accD, accZ, accY,
    r1G, r1U, r1D, r2G, s2G, r2U, s2U, r2D, s2D, rY, sY, rZ, sZ,
    gsum, gsumD, wcol, wcolD, mvcol, mvD, pk, pkr, pk2, nrm, nr1, nr2, mG, mU, vG, vU, mD, vD, kept, reused,
):
    me = lax.axis_index("dp")
    c, k, xy = me % 2, me % COLUMN, me // COLUMN
    z, y, x = k // 2, xy % N, xy // N
    cb = c * NZ + z

    def dev(x, y, z, c):
        return {"dp": ((x * N + y) * NZ + z) * 2 + c}

    def in_column(kk):
        return {"dp": xy * COLUMN + kk}

    partner = dev(x, y, z, 1 - c)
    ring_ids = {
        "x": (dev((x + 1) % N, y, z, c), dev((x + N - 1) % N, y, z, c)),
        "y": (dev(x, (y + 1) % N, z, c), dev(x, (y + N - 1) % N, z, c)),
        "z": (dev(x, y, (z + 1) % NZ, c), dev(x, y, (z + NZ - 1) % NZ, c)),
    }
    counts, used = {"kept": 0, "reused": 0}, []

    def keep():
        counts["kept"] += 1
        return kept.at[counts["kept"] - 1]

    def sem():
        counts["reused"] += 1
        used.append(counts["reused"])
        return reused.at[counts["reused"] - 1]

    def remote(src, dst, ssem, rsem, device):
        return pltpu.make_async_remote_copy(src_ref=src, dst_ref=dst, send_sem=ssem, recv_sem=rsem, device_id=device, device_id_type=MESH)

    sent = []

    def group(ref, new=sem):
        one = new()
        sent.append((one, ref))
        return one

    def drain():
        while sent:
            one, ref = sent.pop(0)
            remote(ref, ref, one, one, partner).wait_send()

    def wait_all(one, ref):
        remote(ref, ref, one, one, partner).wait_recv()

    barrier = pltpu.get_barrier_semaphore()
    for device in (partner, *(one for pair in ring_ids.values() for one in pair)):
        pl.semaphore_signal(barrier, inc=1, device_id=device, device_id_type=MESH)

    def wide(c):
        return pl.ds(pl.multiple_of(c * WIDE, WIDE), WIDE)

    def narrow(c):
        return pl.ds(pl.multiple_of(c * NARROW, NARROW), NARROW)

    def slab(c):
        return pl.ds(pl.multiple_of(c * SLAB, SLAB), SLAB)

    def block(mat, b, c, part):
        if mat == "G":
            return gG.at[:, b, :, part, :, wide(c)]
        if mat == "U":
            return gU.at[:, :, b, part, :, wide(c)]
        return gD.at[:, :, :, b, :, narrow(c)]

    def landing(ref, mat, b, part):
        return ref.at[b] if mat == "D" else ref.at[b, :, :, part]

    own = {"G": ownG, "U": ownU, "D": ownD}
    peer = {"G": peerG, "U": peerU, "D": peerD}
    first = {"G": (x, N), "U": (y, N), "D": (z, NZ)}
    acc = {"G": accG, "U": accU, "D": accD}
    r1 = {"G": r1G, "U": r1U, "D": r1D}
    r2 = {"G": r2G, "U": r2U, "D": r2D}
    s2 = {"G": s2G, "U": s2U, "D": s2D}
    need = []
    for d, offs, part in ((4, (2,), 0), (3, (1, -1), 0), (2, (2,), 1), (1, (1, -1), 1), (0, (2,), 2)):
        need += [("D", off, 0) for off in sorted({d, -d}, reverse=True) if off > -4]
        need += [(mat, off, part) for off in offs for mat in "GU"]
    need += [(mat, 0, 0) for mat in "GU"] + [(mat, off, 2) for off in (1, -1) for mat in "GU"] + [(mat, 0, part) for part in (1, 2) for mat in "GU"]

    def at(mat, off):
        p, n = first[mat]
        return (p + off + n) % n

    loaded = {mat: sem() for mat in own}
    for mat, off, part in need:
        b = at(mat, off)
        pltpu.make_async_copy(block(mat, b, c, part), landing(own[mat], mat, b, part), loaded[mat]).start()
    mine = pl.ds(pl.multiple_of(cb * LANES, LANES), LANES)
    wloads = [pltpu.make_async_copy(w.at[:, x, y, :, :, mine], wcol.at[i], keep()) for i, w in enumerate((wG, wU))]
    wloads.append(pltpu.make_async_copy(wD.at[:, x, y, z, :, narrow(c)], wcolD, keep()))
    mloads = [pltpu.make_async_copy(*pair, sem()) for pair in ((hmG, mG), (hvG, vG), (hmU, mU), (hvU, vU), (hmD, mD), (hvD, vD))]
    for one in mloads + wloads:
        one.start()

    with jax.named_scope("barrier"):
        pl.semaphore_wait(barrier, 7)

    peers, by_mat = {}, {mat: group(own[mat]) for mat in own}
    for mat, off, part in need:
        b = at(mat, off)
        peers[mat, off, part] = remote(block(mat, b, 1 - c, part), landing(peer[mat], mat, b, part), by_mat[mat], sem(), partner)
        peers[mat, off, part].start()

    landed = set()

    def local1(mat, off, b, half, part):
        if mat not in landed:
            landed.add(mat)
            pltpu.make_async_copy(own[mat], own[mat], loaded[mat]).wait()
        if (mat, off, part) not in landed:
            landed.add((mat, off, part))
            peers[mat, off, part].wait_recv()
        return [own[mat].at[b, half], peer[mat].at[b, half]]

    def rs_ring(name, axis, n, pos, local, send, recv, cut, ssem, dims, finish, times):
        seq, copies = order(n), {}
        for i, (far, s) in enumerate(seq):
            prev = seq.index((far, s - 1)) if s > 1 else None
            yield times[i]
            with jax.named_scope(f"{name}_{i}"):
                for d in range(2):
                    half = d if far else 1 - d
                    off = n // 2 - s + far
                    off = -off if d and off < n // 2 else off
                    b = (pos + off + n) % n
                    srcs = [cut(r) for r in local(off, b, half)]
                    if s > 1:
                        copies[d, prev].wait_recv()
                        srcs.append(cut(recv.at[d, prev]))
                    dst = cut(send(d, i, b, half))
                    add_refs(dst, srcs, dims)
                    copies[d, i] = remote(dst, cut(recv.at[d, i]), ssem, sem(), ring_ids[axis][d])
                    copies[d, i].start()
        yield times[-1]
        with jax.named_scope(f"{name}_end"):
            for half in range(2):
                copies[half, n - 2].wait_recv()
                copies[1 - half, n - 3].wait_recv()
                finish(half, [cut(recv.at[half, n - 2]), cut(recv.at[1 - half, n - 3])])

    def stage1(mat, axis, part, cut, ssem, dims, times):
        p, n = first[mat]

        def finish(half, got):
            add_refs(cut(acc[mat].at[half]), [cut(r) for r in local1(mat, 0, p, half, part)] + got, dims)

        return rs_ring(
            "rs" + mat + axis, axis, n, p, lambda off, b, half: local1(mat, off, b, half, part), lambda d, i, b, half: own[mat].at[b, half],
            r1[mat], cut, ssem, dims, finish, times,
        )

    def stage2(mat, axis, pos, cut, ssem, dims, finish, times):
        return rs_ring(
            "rs" + mat + axis, axis, N, pos, lambda off, b, half: [acc[mat].at[half, b]], lambda d, i, b, half: s2[mat].at[d, i],
            r2[mat], cut, ssem, dims, finish, times,
        )

    def to_z(which, mat, pos, part):
        def finish(half, got):
            here = acc[mat].at[half, pos, tiles(part)]

            total = here[0] + got[0][0].astype(F32) + got[1][0].astype(F32)
            for q in range(NZ):
                one = total[:, LANES * q : LANES * q + LANES]
                accZ[q, half, which, part] = one
                sZ[q, half, which, part] = one.astype(BF16)

        return finish

    ss = {key: group(r) for key, r in (("G1", r1G), ("U1", r1U), ("D1", r1D), ("G2", r2G), ("U2", r2U), ("D2", r2D))}
    ss["Z"], ss["Y"] = group(rZ.at[: NZ - 1]), group(rY.at[: N - 1])

    def across_z(part, times):
        got, cut = sem(), tiles(part)
        yield times[0]
        for j in range(1, NZ):
            zz = (z + j) % NZ
            remote(sZ.at[zz, :, :, cut], rZ.at[z, :, :, cut], ss["Z"], got, dev(x, y, zz, c)).start()
        yield times[1]
        with jax.named_scope("rsZ"):
            wait_all(got, rZ.at[: NZ - 1, :, :, cut])

            @pl.loop(0, 2 * LAYERS)
            def _(i):
                half, which = i // 2, i % 2
                total = accZ[z, half, which, part]
                for j in range(1, NZ):
                    total = total + rZ[(z + j) % NZ, half, which, part].astype(F32)
                gsum[half, which, part] = total.astype(BF16).astype(F32)

    def rs_pipe(part, t1, t2, tz):
        cut1, cut2 = (lambda r: r.at[:, tiles(part)]), (lambda r: r.at[tiles(part)])
        long, short = (N, 1), (1,)
        return chain(
            interleave(
                chain(
                    stage1("G", "x", part, cut1, ss["G1"], long, t1),
                    stage2("G", "y", y, cut2, ss["G2"], short, to_z(0, "G", y, part), t2),
                ),
                chain(
                    stage1("U", "y", part, cut1, ss["U1"], long, t1),
                    stage2("U", "x", x, cut2, ss["U2"], short, to_z(1, "U", x, part), t2),
                ),
            ),
            across_z(part, tz),
        )

    def finishDx(half, got):
        @pl.loop(0, N)
        def _(i):
            total = accD[half, x, i] + got[0][i].astype(F32) + got[1][i].astype(F32)
            accY[half, i] = total
            sY[i, half] = total.astype(BF16)

    def across_y(times):
        got = sem()
        yield times[0]
        for j in range(1, N):
            yy = (y + j) % N
            remote(sY.at[yy], rY.at[y], ss["Y"], got, dev(x, yy, z, c)).start()
        yield times[1]
        with jax.named_scope("rsY"):
            wait_all(got, rY.at[: N - 1])
            for half in range(LAYERS):
                total = accY[half, y]
                for j in range(1, N):
                    total = total + rY[(y + j) % N, half].astype(F32)
                gsumD[half] = total.astype(BF16).astype(F32)

    whole = lambda r: r
    mv, mvd = keep(), keep()

    def send_moments():
        yield 16.0
        for one in mloads:
            one.wait()
        for j, ref in enumerate((mG, vG, mU, vU)):
            for l in range(LAYERS):
                for q in range(COLUMN):
                    pk[q, j, TILES * l : TILES * l + TILES, :] = ref[:, l, LANES * q : LANES * q + LANES]
        for j, ref in enumerate((mD, vD)):
            mvD[j, :, slab(c), :] = ref[:, :, narrow(c)]
        yield 33.5
        ssem, ssemD = group(pk.at[: COLUMN - 1]), group(mvD.at[:, :, :SLAB])
        for j in range(1, COLUMN):
            kk = (k + j) % COLUMN
            remote(pk.at[(kk % 2) * NZ + kk // 2], pkr.at[k], ssem, mv, in_column(kk)).start()
        for j, ref in enumerate((mD, vD)):
            remote(ref.at[:, :, narrow(1 - c)], mvD.at[j, :, slab(c)], ssemD, mvd, partner).start()

    run(interleave(
        chain(
            stage1("D", "z", 0, whole, ss["D1"], (N, N), (-1.0, 0.7, 6.7, 10.9, 15.1, 19.3, 23.5, 32.0)),
            stage2("D", "x", x, whole, ss["D2"], (N,), finishDx, (32.0, 32.0, 36.2, 39.5)),
            across_y((39.5, 44.0)),
        ),
        rs_pipe(0, (0.0, 0.8, 5.6, 13.8), (13.9, 13.9, 20.2, 27.2), (27.3, 38.0)),
        rs_pipe(1, (3.0, 8.0, 11.2, 22.2), (22.3, 22.3, 29.0, 33.0), (33.0, 43.0)),
        rs_pipe(2, (10.5, 14.5, 19.6, 28.5), (28.5, 28.5, 34.5, 37.5), (37.5, 46.0)),
        send_moments(),
    ))

    with jax.named_scope("sent"):
        drain()
        counts["reused"] = 0

    with jax.named_scope("norm"):
        total = jnp.zeros((SLAB, LANES), F32)

        def squares(total, g):
            for q in range(g.shape[1] // LANES):
                one = g[:, LANES * q : LANES * q + LANES]
                one = one * one
                total = total + one[:SLAB] + one[SLAB:]
            return total

        for half in range(LAYERS):
            for which in range(2):
                for t in range(TILES):
                    total = squares(total, gsum[half, which, t])
            total = squares(total, gsumD[half])
    for stage, got in enumerate((nr1, nr2)):
        with jax.named_scope(f"norm{stage}"):
            nrm[stage] = total
            here, rsem, ssem = (xy if stage else k), keep(), group(got.at[: COLUMN - 1], keep)
            for j in range(1, COLUMN):
                there = (here + j) % COLUMN
                device = {"dp": there * COLUMN + k} if stage else in_column(there)
                remote(nrm.at[stage], got.at[here], ssem, rsem, device).start()
            if not stage:
                pkr[k] = pk[cb]
                wait_all(mv, pkr.at[: COLUMN - 1])
                for j in range(mvcol.shape[0]):
                    for l in range(LAYERS):
                        for q in range(COLUMN):
                            mvcol[j, l, TILES * q : TILES * q + TILES, :] = pkr[q, j, TILES * l : TILES * l + TILES, :]
                wait_all(mvd, mvD.at[:, :, :SLAB])
                for one in wloads:
                    one.wait()
            got[here] = nrm[stage]
            wait_all(rsem, got.at[: COLUMN - 1])
            total = got[0]
            for j in range(1, COLUMN):
                total = total + got[j]
    total = jnp.sum(jnp.sum(total, axis=1, keepdims=True), axis=0, keepdims=True)
    factor = jnp.minimum(1.0, 0.5 * lax.rsqrt(total / (3 * 2 * 768 * 2048) + 1e-30))

    with jax.named_scope("adamw"):
        for half in range(LAYERS):
            new, m, v = adamw(wcolD[half].astype(F32), mvD[0, half], mvD[1, half], gsumD[half] * factor)
            oD[half, x, y, z, :, narrow(c)] = new
            mvD[0, half] = m
            mvD[1, half] = v
            for a, out in enumerate((oG, oU)):
                for b in range(TILES):
                    rows, at_m, at_v = pl.ds(ROWS * b, ROWS), 2 * a, 2 * a + 1
                    new, m, v = adamw(
                        wcol[a, half, b].astype(F32), mvcol[at_m, half, rows], mvcol[at_v, half, rows], gsum[half, a, b] * factor
                    )
                    out[half, x, y, b, :, mine] = new
                    mvcol[at_m, half, rows] = m
                    mvcol[at_v, half, rows] = v

    onward = {mat: (group(peer[mat]), sem()) for mat in peer}

    def ag_ring(name, axis, n, pos, piece, ssem, on, times):
        seq, copies = order(n), {}

        def pass_on(ref):
            if on:
                remote(ref, ref, *onward[on], partner).start()

        def got(d, i):
            far, s = seq[i]
            copies[d, i].wait_recv()
            pass_on(piece((pos + (s if d else n - s)) % n, d if far else 1 - d))

        for i, (far, s) in enumerate(seq):
            yield times[i]
            with jax.named_scope(f"{name}_{i}"):
                for d in range(2):
                    if s > 1:
                        got(d, seq.index((far, s - 1)))
                    ref = piece((pos + (s - 1 if d else n - s + 1)) % n, d if far else 1 - d)
                    copies[d, i] = remote(ref, ref, ssem, sem(), ring_ids[axis][d])
                    copies[d, i].start()
        for half in range(2):
            pass_on(piece(pos, half))
        for slot in (n - 3, n - 2):
            yield times[slot + 2]
            with jax.named_scope(f"{name}_end{slot}"):
                for d in range(2):
                    got(d, slot)

    others = oD.at[:, :3, 0, :5, :, :NARROW]
    ss = {key: group(r) for key, r in (("G1", r1G), ("U1", r1U), ("D1", r1D), ("G2", r2G), ("U2", r2U), ("D2", others))}
    ss["Z"] = group(rZ.at[: NZ - 1])

    def back_z(part, times):
        got = sem()
        yield times[0]
        for j in range(1, NZ):
            for out in (oG, oU):
                ref = out.at[:, x, y, tiles(part), :, mine]
                remote(ref, ref, ss["Z"], got, dev(x, y, (z + j) % NZ, c)).start()
        yield times[1]
        with jax.named_scope("agZ"):
            wait_all(got, rZ.at[: NZ - 1, :, :, tiles(part)])

    def back_columns(times):
        got = sem()
        yield times[0]
        ref = oD.at[:, x, y, z, :, narrow(c)]
        for j in range(1, COLUMN):
            remote(ref, ref, ss["D2"], got, {"dp": (xy + j) % COLUMN * COLUMN + k}).start()
        yield times[1]
        with jax.named_scope("agXY"):
            wait_all(got, others)

    def ag_pipe(part, tz, t2, t1):
        cols, cut = wide(c), tiles(part)
        return chain(
            back_z(part, tz),
            interleave(
                chain(
                    ag_ring("agGy", "y", N, y, lambda p, half: oG.at[half, x, p, cut, :, cols], ss["G2"], None, t2),
                    ag_ring("agGx", "x", N, x, lambda p, half: oG.at[half, p, :, cut, :, cols], ss["G1"], "G", t1),
                ),
                chain(
                    ag_ring("agUx", "x", N, x, lambda p, half: oU.at[half, p, y, cut, :, cols], ss["U2"], None, t2),
                    ag_ring("agUy", "y", N, y, lambda p, half: oU.at[half, :, p, cut, :, cols], ss["U1"], "U", t1),
                ),
            ),
        )

    rb, rd = keep(), keep()

    def return_moments():
        yield 14.0
        for q in range(COLUMN):
            for j in range(mvcol.shape[0]):
                for l in range(LAYERS):
                    pk2[q, j, TILES * l : TILES * l + TILES, :] = mvcol[j, l, TILES * q : TILES * q + TILES, :]
        ssem, ssemD = group(pk2.at[: COLUMN - 1]), group(backD.at[:, 0])
        for j in range(1, COLUMN):
            kk = (k + j) % COLUMN
            remote(pk2.at[kk], back.at[cb], ssem, rb, in_column(kk)).start()
        for j in range(2):
            remote(mvD.at[j, :, slab(1 - c)], backD.at[j, c], ssemD, rd, partner).start()
            backD[j, c] = mvD[j, :, slab(c)]
        back[cb] = pk2[k]

    run(interleave(
        chain(
            back_columns((0.0, 9.0)),
            ag_ring("agDz", "z", NZ, z, lambda p, half: oD.at[half, :, :, p, :, narrow(c)], ss["D1"], "D",
                    (9.0, 9.0, 15.8, 20.0, 24.2, 28.4, 32.6, 36.8, 41.0)),
        ),
        ag_pipe(0, (0.1, 7.6), (7.6, 7.6, 11.2, 13.4, 14.4), (14.5, 14.5, 20.1, 23.0, 32.0)),
        ag_pipe(1, (0.2, 10.4), (10.4, 10.4, 14.0, 16.5, 17.3), (17.4, 17.4, 26.5, 29.0, 40.2)),
        ag_pipe(2, (0.3, 13.1), (13.1, 13.1, 16.8, 19.2, 23.4), (23.5, 23.5, 34.7, 37.5, 43.0)),
        return_moments(),
    ))

    with jax.named_scope("drain"):
        wait_all(rb, back.at[: COLUMN - 1])
        wait_all(rd, backD.at[:, 0])
        for mat in peer:
            wait_all(onward[mat][1], peer[mat])
        drain()
    assert (counts["kept"], max(used)) == (KEPT, REUSED), (counts["kept"], max(used))


def store(iG, iU, iD, packed, packedD, oG, oU, oD, omG, omU, omD, ovG, ovU, ovD, tmG, tvG, tmU, tvU, tmD, tvD, sem):
    pairs = ((iG, oG), (iU, oU), (iD, oD), (tmG, omG), (tvG, ovG), (tmU, omU), (tvU, ovU), (tmD, omD), (tvD, ovD))
    copies = [pltpu.make_async_copy(*pair, sem.at[j]) for j, pair in enumerate(pairs)]
    for j, (i, o) in enumerate(pairs[:3]):
        for l in range(LAYERS):
            for p in range(N):
                pltpu.make_async_copy(i.at[l, p], o.at[l, p], sem.at[j]).start()
    for j, out in enumerate((tmG, tvG, tmU, tvU)):
        for l in range(LAYERS):
            for q in range(COLUMN):
                out[:, l, LANES * q : LANES * q + LANES] = packed[q, j, TILES * l : TILES * l + TILES, :]
    for j, out in enumerate((tmD, tvD)):
        for h in range(2):
            out[:, :, NARROW * h : NARROW * h + NARROW] = packedD[j, h]
    for one in copies[3:]:
        one.start()
    for one in copies:
        one.wait()


def fused(*arrays):
    g, w, m, v = (arrays[i : i + 3] for i in (0, 3, 6, 9))
    big, low = (N, TILES, ROWS, WIDE), (N, N, ROWS, NARROW)
    view = (LAYERS, N, N, TILES, ROWS, 2 * WIDE)
    views = [view, view, (LAYERS, N, N, NZ, ROWS, 2 * NARROW)]
    g = [one.reshape(s) for one, s in zip(g, views, strict=True)]
    w = [one.reshape(s) for one, s in zip(w, views, strict=True)]
    m, v = ([jnp.swapaxes(one, 0, 1) if one.shape[1] == TILES else one for one in t] for t in (m, v))
    vm, hbm, D = pl.BlockSpec(memory_space=pltpu.VMEM), pl.BlockSpec(memory_space=pl.ANY), pltpu.SemaphoreType.DMA

    def V(dtype, *shape):
        return pltpu.VMEM(shape, dtype)

    tile, packed, packedD = (TILES, ROWS, LANES), (COLUMN, N, SLAB, LANES), (2, 2, LAYERS, SLAB, NARROW)
    moments = [V(F32, *one.shape) for one in (m[0], m[1], v[0], v[1], m[2], v[2])]
    scratch = [
        *[V(BF16, N, LAYERS, *big)] * 4, *[V(BF16, NZ, LAYERS, *low)] * 2,
        *[V(F32, LAYERS, *big)] * 2, V(F32, LAYERS, *low), V(F32, NZ, LAYERS, 2, *tile), V(F32, LAYERS, *low[1:]),
        *[V(BF16, 2, N - 1, *big)] * 2, V(BF16, 2, NZ - 1, *low),
        *[V(BF16, 2, N - 1, *big[1:])] * 4, *[V(BF16, 2, N - 1, *low[1:])] * 2,
        *[V(BF16, N, LAYERS, *low[2:])] * 2, *[V(BF16, NZ, LAYERS, 2, *tile)] * 2,
        V(F32, LAYERS, 2, *tile), V(F32, LAYERS, *low[2:]), V(BF16, 2, LAYERS, *tile), V(BF16, LAYERS, *low[2:]),
        V(F32, N, LAYERS, TILES * ROWS, LANES), V(F32, 2, LAYERS, *low[2:]), *[V(F32, *packed)] * 3,
        V(F32, 2, SLAB, LANES), *[V(F32, COLUMN, SLAB, LANES)] * 2, *moments, D((KEPT,)), D((REUSED,)),
    ]
    passed = pl.pallas_call(
        kernel,
        out_shape=[V(BF16, *s) for s in views] + [V(F32, *packed), V(F32, *packedD)],
        in_specs=[hbm] * 12,
        out_specs=[vm] * 5,
        scratch_shapes=scratch,
        compiler_params=pltpu.CompilerParams(collective_id=0, has_side_effects=True, vmem_limit_bytes=VMEM_LIMIT),
        name="step",
    )(*g, *w, *m, *v)
    outs = pl.pallas_call(
        store,
        out_shape=[jax.ShapeDtypeStruct(s, BF16) for s in views] + [jax.ShapeDtypeStruct(one.shape, F32) for one in (*m, *v)],
        in_specs=[vm] * 5,
        out_specs=[hbm] * 9,
        scratch_shapes=[*(moments[i] for i in (0, 2, 1, 3, 4, 5)), D((9,))],
        compiler_params=pltpu.CompilerParams(vmem_limit_bytes=2**20),
        name="store",
    )(*passed)
    outs = [jnp.swapaxes(o, 0, 1) if o.shape[0] == TILES else o for o in outs]
    return tuple(o.reshape(one.shape) for o, one in zip(outs, (*arrays[3:6], *arrays[6:]), strict=True))


def solution(mesh):
    all_of, cut = P(None, None, None), P(None, "dp", None)
    return jax.shard_map(
        fused,
        mesh=mesh,
        in_specs=(P(("rep", "dp"), None, None, None),) * 3 + (all_of,) * 3 + (cut,) * 6,
        out_specs=(P("rep", None, None),) * 3 + (P("rep", "dp", None),) * 6,
        check_vma=False,
    )
```

```python
import math

import jax
import jax.numpy as jnp
from jax import lax
from jax.experimental import pallas as pl
from jax.experimental.pallas import tpu as pltpu
from jax.sharding import PartitionSpec as P

N, NZ, COLUMN = 4, 8, 16
LAYERS, ROWS, LANES = 2, 16, 128
TILES, WIDE, NARROW = 3, 1024, 384
SLAB = 8
F32, BF16 = jnp.float32, jnp.bfloat16
MESH = pl.DeviceIdType.MESH
KEPT, REUSED = 11, 95
VMEM_LIMIT = 36 * 2**20


def add_refs(dst, srcs, dims):
    @pl.loop(0, math.prod(dims))
    def _(i):
        at = []
        for d in reversed(dims):
            at.insert(0, i % d)
            i = i // d
        at = tuple(at)
        total = srcs[0][at].astype(F32)
        for s in srcs[1:]:
            total = total + s[at].astype(F32)
        dst[at] = total.astype(dst.dtype)


def order(n):
    half, seq = n // 2, []
    for s in range(1, half + 1):
        seq.append((True, s))
        if s < half:
            seq.append((False, s))
    return seq


def interleave(*some):
    live = [[next(r), r] for r in some]
    while live:
        first = min(live, key=lambda o: o[0])
        yield first[0]
        first[0] = next(first[1], None)
        if first[0] is None:
            live.remove(first)


def chain(*some):
    for one in some:
        yield from one


def run(generator):
    for _ in generator:
        pass


def packed_rows(j, l):
    start = (j * LAYERS + l) * TILES
    return slice(start, start + TILES)


def tiles(part):
    return pl.ds(part, 1)


def adamw(w, m, v, g):
    m = 0.9 * m + 0.1 * g
    v = 0.95 * v + 0.05 * g * g
    step = m * lax.rsqrt(v + 1e-8) + 0.1 * w
    return (w - 0.02 * step).astype(BF16), m, v


def kernel(
    gG, gU, gD, wG, wU, wD, hmG, hmU, hmD, hvG, hvU, hvD, oG, oU, oD, back, backD,
    ownG, peerG, ownU, peerU, ownD, peerD, accG, accU, accD, accZ, accY,
    r1G, r1U, r1D, r2G, s2G, r2U, s2U, r2D, s2D, rY, sY, rZ, sZ,
    gsum, gsumD, wcol, wcolD, mvcol, mvD, pk, pkr, pk2, nrm, nr1, nr2, mG, mU, vG, vU, mD, vD, kept, reused,
):
    me = lax.axis_index("dp")
    c, k, xy = me % 2, me % COLUMN, me // COLUMN
    z, y, x = k // 2, xy % N, xy // N
    cb = c * NZ + z

    def dev(x, y, z, c):
        return {"dp": ((x * N + y) * NZ + z) * 2 + c}

    def in_column(kk):
        return {"dp": xy * COLUMN + kk}

    partner = dev(x, y, z, 1 - c)
    ring_ids = {
        "x": (dev((x + 1) % N, y, z, c), dev((x + N - 1) % N, y, z, c)),
        "y": (dev(x, (y + 1) % N, z, c), dev(x, (y + N - 1) % N, z, c)),
        "z": (dev(x, y, (z + 1) % NZ, c), dev(x, y, (z + NZ - 1) % NZ, c)),
    }
    counts, used = {"kept": 0, "reused": 0}, []

    def keep():
        counts["kept"] += 1
        return kept.at[counts["kept"] - 1]

    def sem():
        counts["reused"] += 1
        used.append(counts["reused"])
        return reused.at[counts["reused"] - 1]

    def remote(src, dst, ssem, rsem, device):
        return pltpu.make_async_remote_copy(src_ref=src, dst_ref=dst, send_sem=ssem, recv_sem=rsem, device_id=device, device_id_type=MESH)

    sent = []

    def group(ref, new=sem):
        one = new()
        sent.append((one, ref))
        return one

    def drain():
        while sent:
            one, ref = sent.pop(0)
            remote(ref, ref, one, one, partner).wait_send()

    def wait_all(one, ref):
        remote(ref, ref, one, one, partner).wait_recv()

    barrier = pltpu.get_barrier_semaphore()
    for device in (partner, *(one for pair in ring_ids.values() for one in pair)):
        pl.semaphore_signal(barrier, inc=1, device_id=device, device_id_type=MESH)

    def wide(c):
        return pl.ds(pl.multiple_of(c * WIDE, WIDE), WIDE)

    def narrow(c):
        return pl.ds(pl.multiple_of(c * NARROW, NARROW), NARROW)

    def slab(c):
        return pl.ds(pl.multiple_of(c * SLAB, SLAB), SLAB)

    def block(mat, b, c, part):
        if mat == "G":
            return gG.at[:, b, :, part, :, wide(c)]
        if mat == "U":
            return gU.at[:, :, b, part, :, wide(c)]
        return gD.at[:, :, :, b, :, narrow(c)]

    def landing(ref, mat, b, part):
        return ref.at[b] if mat == "D" else ref.at[b, :, :, part]

    own = {"G": ownG, "U": ownU, "D": ownD}
    peer = {"G": peerG, "U": peerU, "D": peerD}
    first = {"G": (x, N), "U": (y, N), "D": (z, NZ)}
    acc = {"G": accG, "U": accU, "D": accD}
    r1 = {"G": r1G, "U": r1U, "D": r1D}
    r2 = {"G": r2G, "U": r2U, "D": r2D}
    s2 = {"G": s2G, "U": s2U, "D": s2D}
    need = []
    for d, offs, part in ((4, (2,), 0), (3, (1, -1), 0), (2, (2,), 1), (1, (1, -1), 1), (0, (2,), 2)):
        need += [("D", off, 0) for off in sorted({d, -d}, reverse=True) if off > -4]
        need += [(mat, off, part) for off in offs for mat in "GU"]
    need += [(mat, 0, 0) for mat in "GU"] + [(mat, off, 2) for off in (1, -1) for mat in "GU"] + [(mat, 0, part) for part in (1, 2) for mat in "GU"]

    def at(mat, off):
        p, n = first[mat]
        return (p + off + n) % n

    loaded = {mat: sem() for mat in own}
    for mat, off, part in need:
        b = at(mat, off)
        pltpu.make_async_copy(block(mat, b, c, part), landing(own[mat], mat, b, part), loaded[mat]).start()
    mine = pl.ds(pl.multiple_of(cb * LANES, LANES), LANES)
    wloads = [pltpu.make_async_copy(w.at[:, x, y, :, :, mine], wcol.at[i], keep()) for i, w in enumerate((wG, wU))]
    wloads.append(pltpu.make_async_copy(wD.at[:, x, y, z, :, narrow(c)], wcolD, keep()))
    mloads = [pltpu.make_async_copy(*pair, sem()) for pair in ((hmG, mG), (hvG, vG), (hmU, mU), (hvU, vU), (hmD, mD), (hvD, vD))]
    for one in mloads + wloads:
        one.start()

    with jax.named_scope("barrier"):
        pl.semaphore_wait(barrier, 7)

    peers, by_mat = {}, {mat: group(own[mat]) for mat in own}
    for mat, off, part in need:
        b, key = at(mat, off), (mat, abs(off), part)
        if key not in peers:
            peers[key] = sem()
        remote(block(mat, b, 1 - c, part), landing(peer[mat], mat, b, part), by_mat[mat], peers[key], partner).start()

    landed = set()

    def local1(mat, off, b, half, part):
        if mat not in landed:
            landed.add(mat)
            pltpu.make_async_copy(own[mat], own[mat], loaded[mat]).wait()
        key = mat, abs(off), part
        if key not in landed:
            landed.add(key)
            some = slice(0, 1 if off in (0, first[mat][1] // 2) else 2)
            wait_all(peers[key], peer[mat].at[some] if mat == "D" else peer[mat].at[some, :, :, part])
        return [own[mat].at[b, half], peer[mat].at[b, half]]

    def rs_ring(name, axis, n, pos, local, send, recv, index, ssem, dims, finish, times):
        seq, landing_sems = order(n), []

        def cut(ref):
            return ref.at[index] if index else ref

        def wait_both(slot):
            wait_all(landing_sems[slot], recv.at[(slice(None), slot, *index)])

        for i, (far, s) in enumerate(seq):
            prev = seq.index((far, s - 1)) if s > 1 else None
            yield times[i]
            with jax.named_scope(f"{name}_{i}"):
                landing_sems.append(sem())
                if s > 1:
                    wait_both(prev)
                for d in range(2):
                    half = d if far else 1 - d
                    off = n // 2 - s + far
                    off = -off if d and off < n // 2 else off
                    b = (pos + off + n) % n
                    srcs = [cut(r) for r in local(off, b, half)]
                    if s > 1:
                        srcs.append(cut(recv.at[d, prev]))
                    dst = cut(send(d, i, b, half))
                    add_refs(dst, srcs, dims)
                    remote(dst, cut(recv.at[d, i]), ssem, landing_sems[i], ring_ids[axis][d]).start()
        yield times[-1]
        with jax.named_scope(f"{name}_end"):
            wait_both(n - 3)
            wait_both(n - 2)
            for half in range(2):
                finish(half, [cut(recv.at[half, n - 2]), cut(recv.at[1 - half, n - 3])])

    def stage1(mat, axis, part, index, ssem, dims, times):
        p, n = first[mat]

        def cut(ref):
            return ref.at[index] if index else ref

        def finish(half, got):
            add_refs(cut(acc[mat].at[half]), [cut(r) for r in local1(mat, 0, p, half, part)] + got, dims)

        return rs_ring(
            "rs" + mat + axis, axis, n, p, lambda off, b, half: local1(mat, off, b, half, part), lambda d, i, b, half: own[mat].at[b, half],
            r1[mat], index, ssem, dims, finish, times,
        )

    def stage2(mat, axis, pos, index, ssem, dims, finish, times):
        return rs_ring(
            "rs" + mat + axis, axis, N, pos, lambda off, b, half: [acc[mat].at[half, b]], lambda d, i, b, half: s2[mat].at[d, i],
            r2[mat], index, ssem, dims, finish, times,
        )

    def to_z(which, mat, pos, part):
        def finish(half, got):
            here = acc[mat].at[half, pos, tiles(part)]

            total = here[0] + got[0][0].astype(F32) + got[1][0].astype(F32)
            for q in range(NZ):
                one = total[:, LANES * q : LANES * q + LANES]
                accZ[q, half, which, part] = one
                sZ[q, half, which, part] = one.astype(BF16)

        return finish

    ss = {key: group(r) for key, r in (("G1", r1G), ("U1", r1U), ("D1", r1D), ("G2", r2G), ("U2", r2U), ("D2", r2D))}
    ss["Z"], ss["Y"] = group(rZ.at[: NZ - 1]), group(rY.at[: N - 1])

    def across_z(part, times):
        got, cut = sem(), tiles(part)
        yield times[0]
        for j in range(1, NZ):
            zz = (z + j) % NZ
            remote(sZ.at[zz, :, :, cut], rZ.at[z, :, :, cut], ss["Z"], got, dev(x, y, zz, c)).start()
        yield times[1]
        with jax.named_scope("rsZ"):
            wait_all(got, rZ.at[: NZ - 1, :, :, cut])

            @pl.loop(0, 2 * LAYERS)
            def _(i):
                half, which = i // 2, i % 2
                total = accZ[z, half, which, part]
                for j in range(1, NZ):
                    total = total + rZ[(z + j) % NZ, half, which, part].astype(F32)
                gsum[half, which, part] = total.astype(BF16).astype(F32)

    def rs_pipe(part, tG, tU, tz):
        cut1, cut2 = (slice(None), tiles(part)), (tiles(part),)
        long, short = (N, 1), (1,)
        return chain(
            interleave(
                chain(
                    stage1("G", "x", part, cut1, ss["G1"], long, tG[:N]),
                    stage2("G", "y", y, cut2, ss["G2"], short, to_z(0, "G", y, part), tG[N:]),
                ),
                chain(
                    stage1("U", "y", part, cut1, ss["U1"], long, tU[:N]),
                    stage2("U", "x", x, cut2, ss["U2"], short, to_z(1, "U", x, part), tU[N:]),
                ),
            ),
            across_z(part, tz),
        )

    def finishDx(half, got):
        @pl.loop(0, N)
        def _(i):
            total = accD[half, x, i] + got[0][i].astype(F32) + got[1][i].astype(F32)
            accY[half, i] = total
            sY[i, half] = total.astype(BF16)

    def across_y(times):
        got = sem()
        yield times[0]
        for j in range(1, N):
            yy = (y + j) % N
            remote(sY.at[yy], rY.at[y], ss["Y"], got, dev(x, yy, z, c)).start()
        yield times[1]
        with jax.named_scope("rsY"):
            wait_all(got, rY.at[: N - 1])
            for half in range(LAYERS):
                total = accY[half, y]
                for j in range(1, N):
                    total = total + rY[(y + j) % N, half].astype(F32)
                gsumD[half] = total.astype(BF16).astype(F32)

    mv, mvd = keep(), keep()

    def send_moments():
        yield 11.5
        for one in mloads:
            one.wait()
        for j, ref in enumerate((mG, vG, mU, vU)):
            for l in range(LAYERS):
                for q in range(COLUMN):
                    pk[q, packed_rows(j, l), :] = ref[:, l, LANES * q : LANES * q + LANES]
        for j, ref in enumerate((mD, vD)):
            mvD[j, :, slab(c), :] = ref[:, :, narrow(c)]
        yield 61.5
        ssem, ssemD = group(pk.at[: COLUMN - 1]), group(mvD.at[:, :, :SLAB])
        for j in range(1, COLUMN):
            kk = (k + j) % COLUMN
            remote(pk.at[(kk % 2) * NZ + kk // 2], pkr.at[k], ssem, mv, in_column(kk)).start()
        for j, ref in enumerate((mD, vD)):
            remote(ref.at[:, :, narrow(1 - c)], mvD.at[j, :, slab(c)], ssemD, mvd, partner).start()

    run(interleave(
        chain(
            stage1("D", "z", 0, (), ss["D1"], (N, N), (0, 5, 10, 12, 18, 22, 30, 50)),
            stage2("D", "x", x, (), ss["D2"], (N,), finishDx, (51, 54, 59, 63)),
            across_y((64, 66)),
        ),
        rs_pipe(0, (1, 3, 8, 16, 33, 38, 46, 55), (2, 4, 9, 17, 34, 37, 47, 56), (57, 65)),
        rs_pipe(1, (6, 11, 15, 25, 28, 35, 36, 48), (7, 13, 14, 24, 26, 31, 32, 44), (49, 62)),
        rs_pipe(2, (19, 21, 27, 39, 40, 43, 52, 58), (20, 23, 29, 41, 42, 45, 53, 60), (61, 67)),
        send_moments(),
    ))

    with jax.named_scope("sent"):
        drain()
        counts["reused"] = 0

    with jax.named_scope("norm"):
        total = jnp.zeros((SLAB, LANES), F32)

        def squares(total, g):
            for q in range(g.shape[1] // LANES):
                one = g[:, LANES * q : LANES * q + LANES]
                one = one * one
                total = total + one[:SLAB] + one[SLAB:]
            return total

        for half in range(LAYERS):
            for which in range(2):
                for t in range(TILES):
                    total = squares(total, gsum[half, which, t])
            total = squares(total, gsumD[half])
        total = jnp.sum(total, axis=0, keepdims=True)
    for stage, got in enumerate((nr1, nr2)):
        with jax.named_scope(f"norm{stage}"):
            nrm[stage] = total
            here, rsem, ssem = (xy if stage else k), keep(), group(got.at[: COLUMN - 1], keep)
            for j in range(1, COLUMN):
                there = (here + j) % COLUMN
                device = {"dp": there * COLUMN + k} if stage else in_column(there)
                remote(nrm.at[stage], got.at[here], ssem, rsem, device).start()
            if not stage:
                pkr[k] = pk[cb]
                wait_all(mv, pkr.at[: COLUMN - 1])
                for j in range(mvcol.shape[0]):
                    for l in range(LAYERS):
                        for q in range(COLUMN):
                            mvcol[j, l, TILES * q : TILES * q + TILES, :] = pkr[q, packed_rows(j, l), :]
                wait_all(mvd, mvD.at[:, :, :SLAB])
                for one in wloads:
                    one.wait()
            got[here] = nrm[stage]
            wait_all(rsem, got.at[: COLUMN - 1])
            total = got[0]
            for j in range(1, COLUMN):
                total = total + got[j]
    total = jnp.sum(total, axis=1, keepdims=True)
    factor = jnp.minimum(1.0, 0.5 * lax.rsqrt(total / (3 * 2 * 768 * 2048) + 1e-30))

    with jax.named_scope("adamw"):
        for half in range(LAYERS):
            new, m, v = adamw(wcolD[half].astype(F32), mvD[0, half], mvD[1, half], gsumD[half] * factor)
            oD[half, x, y, z, :, narrow(c)] = new
            mvD[0, half] = m
            mvD[1, half] = v
            for a, out in enumerate((oG, oU)):
                for b in range(TILES):
                    rows, at_m, at_v = pl.ds(ROWS * b, ROWS), 2 * a, 2 * a + 1
                    new, m, v = adamw(
                        wcol[a, half, b].astype(F32), mvcol[at_m, half, rows], mvcol[at_v, half, rows], gsum[half, a, b] * factor
                    )
                    out[half, x, y, b, :, mine] = new
                    mvcol[at_m, half, rows] = m
                    mvcol[at_v, half, rows] = v

    onward = {mat: (group(peer[mat]), sem()) for mat in peer}

    def ag_ring(name, axis, n, pos, piece, two, ssem, on, times):
        seq, landing_sems = order(n), []

        def pass_on(ref):
            if on:
                remote(ref, ref, *onward[on], partner).start()

        def got(i):
            far, s = seq[i]
            wait_all(landing_sems[i], two)
            for d in range(2):
                pass_on(piece((pos + (s if d else n - s)) % n, d if far else 1 - d))

        for i, (far, s) in enumerate(seq):
            yield times[i]
            with jax.named_scope(f"{name}_{i}"):
                landing_sems.append(sem())
                if s > 1:
                    got(seq.index((far, s - 1)))
                for d in range(2):
                    ref = piece((pos + (s - 1 if d else n - s + 1)) % n, d if far else 1 - d)
                    remote(ref, ref, ssem, landing_sems[i], ring_ids[axis][d]).start()
        for half in range(2):
            pass_on(piece(pos, half))
        for slot in (n - 3, n - 2):
            yield times[slot + 2]
            with jax.named_scope(f"{name}_end{slot}"):
                got(slot)

    others = oD.at[:, :3, 0, :5, :, :NARROW]
    ss = {key: group(r) for key, r in (("G1", r1G), ("U1", r1U), ("D1", r1D), ("G2", r2G), ("U2", r2U), ("D2", others))}
    ss["Z"] = group(rZ.at[: NZ - 1])

    def back_z(part, times):
        got = sem()
        yield times[0]
        for j in range(1, NZ):
            for out in (oG, oU):
                ref = out.at[:, x, y, tiles(part), :, mine]
                remote(ref, ref, ss["Z"], got, dev(x, y, (z + j) % NZ, c)).start()
        yield times[1]
        with jax.named_scope("agZ"):
            wait_all(got, rZ.at[: NZ - 1, :, :, tiles(part)])

    def back_columns(times):
        got = sem()
        yield times[0]
        ref = oD.at[:, x, y, z, :, narrow(c)]
        for j in range(1, COLUMN):
            remote(ref, ref, ss["D2"], got, {"dp": (xy + j) % COLUMN * COLUMN + k}).start()
        yield times[1]
        with jax.named_scope("agXY"):
            wait_all(got, others)

    def ag_pipe(part, tz, tG, tU):
        cols, cut, n = wide(c), tiles(part), N + 1
        two1, two2 = r1G.at[:, 0, :, cut], r2G.at[:, 0, cut]
        return chain(
            back_z(part, tz),
            interleave(
                chain(
                    ag_ring("agGy", "y", N, y, lambda p, half: oG.at[half, x, p, cut, :, cols], two2, ss["G2"], None, tG[:n]),
                    ag_ring("agGx", "x", N, x, lambda p, half: oG.at[half, p, :, cut, :, cols], two1, ss["G1"], "G", tG[n:]),
                ),
                chain(
                    ag_ring("agUx", "x", N, x, lambda p, half: oU.at[half, p, y, cut, :, cols], two2, ss["U2"], None, tU[:n]),
                    ag_ring("agUy", "y", N, y, lambda p, half: oU.at[half, :, p, cut, :, cols], two1, ss["U1"], "U", tU[n:]),
                ),
            ),
        )

    rb, rd = keep(), keep()

    def return_moments():
        yield 3
        for q in range(COLUMN):
            for j in range(mvcol.shape[0]):
                for l in range(LAYERS):
                    pk2[q, packed_rows(j, l), :] = mvcol[j, l, TILES * q : TILES * q + TILES, :]
        ssem, ssemD = group(pk2.at[: COLUMN - 1]), group(backD.at[:, 0])
        for j in range(1, COLUMN):
            kk = (k + j) % COLUMN
            remote(pk2.at[kk], back.at[cb], ssem, rb, in_column(kk)).start()
        for j in range(2):
            remote(mvD.at[j, :, slab(1 - c)], backD.at[j, c], ssemD, rd, partner).start()
            backD[j, c] = mvD[j, :, slab(c)]
        back[cb] = pk2[k]

    run(interleave(
        chain(
            back_columns((4, 17)),
            ag_ring("agDz", "z", NZ, z, lambda p, half: oD.at[half, :, :, p, :, narrow(c)], r1D.at[:, 0], ss["D1"], "D", (20, 34, 44, 51, 56, 61, 70, 73, 78)),
        ),
        ag_pipe(0, (2, 21), (23, 25, 36, 38, 48, 49, 57, 59, 68, 71), (22, 24, 35, 37, 47, 50, 58, 60, 69, 72)),
        ag_pipe(1, (0, 5), (7, 9, 16, 19, 32, 33, 64, 65, 74, 76), (6, 8, 15, 18, 30, 31, 66, 67, 75, 77)),
        ag_pipe(2, (1, 10), (12, 14, 27, 29, 41, 42, 45, 52, 54, 62), (11, 13, 26, 28, 40, 43, 46, 53, 55, 63)),
        return_moments(),
    ))

    with jax.named_scope("drain"):
        wait_all(rb, back.at[: COLUMN - 1])
        wait_all(rd, backD.at[:, 0])
        for mat in peer:
            wait_all(onward[mat][1], peer[mat])
        drain()
    assert (counts["kept"], max(used)) == (KEPT, REUSED), (counts["kept"], max(used))


def store(iG, iU, iD, packed, packedD, oG, oU, oD, omG, omU, omD, ovG, ovU, ovD, tmG, tvG, tmU, tvU, tmD, tvD, sem):
    pairs = ((iG, oG), (iU, oU), (iD, oD), (tmG, omG), (tvG, ovG), (tmU, omU), (tvU, ovU), (tmD, omD), (tvD, ovD))
    copies = [pltpu.make_async_copy(*pair, sem.at[j]) for j, pair in enumerate(pairs)]
    for j, (i, o) in enumerate(pairs[:3]):
        for l in range(LAYERS):
            for p in range(N):
                pltpu.make_async_copy(i.at[l, p], o.at[l, p], sem.at[j]).start()
    for j, out in enumerate((tmG, tvG, tmU, tvU)):
        for l in range(LAYERS):
            for q in range(COLUMN):
                out[:, l, LANES * q : LANES * q + LANES] = packed[q, packed_rows(j, l), :]
    for j, out in enumerate((tmD, tvD)):
        for h in range(2):
            out[:, :, NARROW * h : NARROW * h + NARROW] = packedD[j, h]
    for one in copies[3:]:
        one.start()
    for one in copies:
        one.wait()


def fused(*arrays):
    g, w, m, v = (arrays[i : i + 3] for i in (0, 3, 6, 9))
    big, low = (N, TILES, ROWS, WIDE), (N, N, ROWS, NARROW)
    view = (LAYERS, N, N, TILES, ROWS, 2 * WIDE)
    views = [view, view, (LAYERS, N, N, NZ, ROWS, 2 * NARROW)]
    g = [one.reshape(s) for one, s in zip(g, views, strict=True)]
    w = [one.reshape(s) for one, s in zip(w, views, strict=True)]
    m, v = ([jnp.swapaxes(one, 0, 1) if one.shape[1] == TILES else one for one in t] for t in (m, v))
    vm, hbm, D = pl.BlockSpec(memory_space=pltpu.VMEM), pl.BlockSpec(memory_space=pl.ANY), pltpu.SemaphoreType.DMA

    def V(dtype, *shape):
        return pltpu.VMEM(shape, dtype)

    tile, packed, packedD = (TILES, ROWS, LANES), (COLUMN, N * LAYERS * TILES, LANES), (2, 2, LAYERS, SLAB, NARROW)
    moments = [V(F32, *one.shape) for one in (m[0], m[1], v[0], v[1], m[2], v[2])]
    scratch = [
        *[V(BF16, N, LAYERS, *big)] * 4, *[V(BF16, NZ, LAYERS, *low)] * 2,
        *[V(F32, LAYERS, *big)] * 2, V(F32, LAYERS, *low), V(F32, NZ, LAYERS, 2, *tile), V(F32, LAYERS, *low[1:]),
        *[V(BF16, 2, N - 1, *big)] * 2, V(BF16, 2, NZ - 1, *low),
        *[V(BF16, 2, N - 1, *big[1:])] * 4, *[V(BF16, 2, N - 1, *low[1:])] * 2,
        *[V(BF16, N, LAYERS, *low[2:])] * 2, *[V(BF16, NZ, LAYERS, 2, *tile)] * 2,
        V(F32, LAYERS, 2, *tile), V(F32, LAYERS, *low[2:]), V(BF16, 2, LAYERS, *tile), V(BF16, LAYERS, *low[2:]),
        V(F32, N, LAYERS, TILES * ROWS, LANES), V(F32, 2, LAYERS, *low[2:]), *[V(F32, *packed)] * 3,
        V(F32, 2, 1, LANES), *[V(F32, COLUMN, 1, LANES)] * 2, *moments, D((KEPT,)), D((REUSED,)),
    ]
    passed = pl.pallas_call(
        kernel,
        out_shape=[V(BF16, *s) for s in views] + [V(F32, *packed), V(F32, *packedD)],
        in_specs=[hbm] * 12,
        out_specs=[vm] * 5,
        scratch_shapes=scratch,
        compiler_params=pltpu.CompilerParams(collective_id=0, has_side_effects=True, vmem_limit_bytes=VMEM_LIMIT),
        name="step",
    )(*g, *w, *m, *v)
    outs = pl.pallas_call(
        store,
        out_shape=[jax.ShapeDtypeStruct(s, BF16) for s in views] + [jax.ShapeDtypeStruct(one.shape, F32) for one in (*m, *v)],
        in_specs=[vm] * 5,
        out_specs=[hbm] * 9,
        scratch_shapes=[*(moments[i] for i in (0, 2, 1, 3, 4, 5)), D((9,))],
        compiler_params=pltpu.CompilerParams(vmem_limit_bytes=2**20),
        name="store",
    )(*passed)
    outs = [jnp.swapaxes(o, 0, 1) if o.shape[0] == TILES else o for o in outs]
    return tuple(o.reshape(one.shape) for o, one in zip(outs, (*arrays[3:6], *arrays[6:]), strict=True))


def solution(mesh):
    all_of, cut = P(None, None, None), P(None, "dp", None)
    return jax.shard_map(
        fused,
        mesh=mesh,
        in_specs=(P(("rep", "dp"), None, None, None),) * 3 + (all_of,) * 3 + (cut,) * 6,
        out_specs=(P("rep", None, None),) * 3 + (P("rep", "dp", None),) * 6,
        check_vma=False,
    )
```

```python
import math

import jax
import jax.numpy as jnp
from jax import lax
from jax.experimental import pallas as pl
from jax.experimental.pallas import tpu as pltpu
from jax.sharding import PartitionSpec as P

N, NZ, COLUMN = 4, 8, 16
LAYERS, ROWS, LANES = 2, 16, 128
TILES, WIDE, NARROW = 3, 1024, 384
SLAB = 8
F32, BF16 = jnp.float32, jnp.bfloat16
MESH = pl.DeviceIdType.MESH
KEPT, REUSED = 13, 98
VMEM_LIMIT = 36 * 2**20


def add_refs(dst, srcs, dims):
    @pl.loop(0, math.prod(dims))
    def _(i):
        at = []
        for d in reversed(dims):
            at.insert(0, i % d)
            i = i // d
        at = tuple(at)
        total = srcs[0][at].astype(F32)
        for s in srcs[1:]:
            total = total + s[at].astype(F32)
        dst[at] = total.astype(dst.dtype)


def order(n):
    half, seq = n // 2, []
    for s in range(1, half + 1):
        seq.append((True, s))
        if s < half:
            seq.append((False, s))
    return seq


def interleave(*some):
    live = [[next(r), r] for r in some]
    while live:
        first = min(live, key=lambda o: o[0])
        yield first[0]
        first[0] = next(first[1], None)
        if first[0] is None:
            live.remove(first)


def chain(*some):
    for one in some:
        yield from one


def run(generator):
    for _ in generator:
        pass


def packed_rows(j, l):
    start = (j * LAYERS + l) * TILES
    return slice(start, start + TILES)


def tiles(part):
    return pl.ds(part, 1)


def adamw(w, m, v, g):
    m, v = moments(m, v, g)
    step = m * lax.rsqrt(v + 1e-8) + 0.1 * w
    return (w - 0.02 * step).astype(BF16), m, v


def moments(m, v, g):
    return 0.9 * m + 0.1 * g, 0.95 * v + 0.05 * g * g


def kernel(
    gG, gU, gD, wG, wU, wD, hmG, hmU, hmD, hvG, hvU, hvD, oG, oU, oD, omG, omU, omD, ovG, ovU, ovD,
    ownG, peerG, ownU, peerU, ownD, peerD, accG, accU, accD, accZ, accY,
    r1G, r1U, r1D, r2G, s2G, r2U, s2U, r2D, s2D, rY, sY, rZ, sZ,
    gsum, gsumD, wcol, wcolD, mvcol, mvD, pk, pkr, gk, gr, gkD, nrm, nr1, nr2, mG, mU, vG, vU, mD, vD, kept, reused,
):
    me = lax.axis_index("dp")
    c, k, xy = me % 2, me % COLUMN, me // COLUMN
    z, y, x = k // 2, xy % N, xy // N
    cb = c * NZ + z

    def dev(x, y, z, c):
        return {"dp": ((x * N + y) * NZ + z) * 2 + c}

    def in_column(kk):
        return {"dp": xy * COLUMN + kk}

    partner = dev(x, y, z, 1 - c)
    ring_ids = {
        "x": (dev((x + 1) % N, y, z, c), dev((x + N - 1) % N, y, z, c)),
        "y": (dev(x, (y + 1) % N, z, c), dev(x, (y + N - 1) % N, z, c)),
        "z": (dev(x, y, (z + 1) % NZ, c), dev(x, y, (z + NZ - 1) % NZ, c)),
    }
    counts, used = {"kept": 0, "reused": 0}, []

    def keep():
        counts["kept"] += 1
        return kept.at[counts["kept"] - 1]

    def sem():
        counts["reused"] += 1
        used.append(counts["reused"])
        return reused.at[counts["reused"] - 1]

    def remote(src, dst, ssem, rsem, device):
        return pltpu.make_async_remote_copy(src_ref=src, dst_ref=dst, send_sem=ssem, recv_sem=rsem, device_id=device, device_id_type=MESH)

    sent = []

    def group(ref, new=sem):
        one = new()
        sent.append((one, ref))
        return one

    def drain():
        while sent:
            one, ref = sent.pop(0)
            remote(ref, ref, one, one, partner).wait_send()

    def wait_all(one, ref):
        remote(ref, ref, one, one, partner).wait_recv()

    barrier = pltpu.get_barrier_semaphore()
    for device in (partner, *(one for pair in ring_ids.values() for one in pair)):
        pl.semaphore_signal(barrier, inc=1, device_id=device, device_id_type=MESH)

    def wide(c):
        return pl.ds(pl.multiple_of(c * WIDE, WIDE), WIDE)

    def narrow(c):
        return pl.ds(pl.multiple_of(c * NARROW, NARROW), NARROW)

    def slab(c):
        return pl.ds(pl.multiple_of(c * SLAB, SLAB), SLAB)

    def block(mat, b, c, part):
        if mat == "G":
            return gG.at[:, b, :, part, :, wide(c)]
        if mat == "U":
            return gU.at[:, :, b, part, :, wide(c)]
        return gD.at[:, :, :, b, :, narrow(c)]

    def landing(ref, mat, b, part):
        return ref.at[b] if mat == "D" else ref.at[b, :, :, part]

    own = {"G": ownG, "U": ownU, "D": ownD}
    peer = {"G": peerG, "U": peerU, "D": peerD}
    first = {"G": (x, N), "U": (y, N), "D": (z, NZ)}
    acc = {"G": accG, "U": accU, "D": accD}
    r1 = {"G": r1G, "U": r1U, "D": r1D}
    r2 = {"G": r2G, "U": r2U, "D": r2D}
    s2 = {"G": s2G, "U": s2U, "D": s2D}
    need = []
    for d, offs, part in ((4, (2,), 0), (3, (1, -1), 0), (2, (2,), 1), (1, (1, -1), 1), (0, (2,), 2)):
        need += [("D", off, 0) for off in sorted({d, -d}, reverse=True) if off > -4]
        need += [(mat, off, part) for off in offs for mat in "GU"]
    need += [(mat, 0, 0) for mat in "GU"] + [(mat, off, 2) for off in (1, -1) for mat in "GU"] + [(mat, 0, part) for part in (1, 2) for mat in "GU"]

    def at(mat, off):
        p, n = first[mat]
        return (p + off + n) % n

    loaded = {mat: sem() for mat in own}
    for mat, off, part in need:
        b = at(mat, off)
        pltpu.make_async_copy(block(mat, b, c, part), landing(own[mat], mat, b, part), loaded[mat]).start()
    mine = pl.ds(pl.multiple_of(cb * LANES, LANES), LANES)
    wloads = [pltpu.make_async_copy(w.at[:, x, y, :, :, mine], wcol.at[i], keep()) for i, w in enumerate((wG, wU))]
    wloads.append(pltpu.make_async_copy(wD.at[:, x, y, z, :, narrow(c)], wcolD, keep()))
    mloads = [pltpu.make_async_copy(*pair, sem()) for pair in ((hmG, mG), (hvG, vG), (hmU, mU), (hvU, vU), (hmD, mD), (hvD, vD))]
    for one in mloads + wloads:
        one.start()

    with jax.named_scope("barrier"):
        pl.semaphore_wait(barrier, 7)

    peers, by_mat = {}, {mat: group(own[mat]) for mat in own}
    for mat, off, part in need:
        b, key = at(mat, off), (mat, abs(off), part)
        if key not in peers:
            peers[key] = sem()
        remote(block(mat, b, 1 - c, part), landing(peer[mat], mat, b, part), by_mat[mat], peers[key], partner).start()

    landed = set()

    def local1(mat, off, b, half, part):
        if mat not in landed:
            landed.add(mat)
            pltpu.make_async_copy(own[mat], own[mat], loaded[mat]).wait()
        key = mat, abs(off), part
        if key not in landed:
            landed.add(key)
            some = slice(0, 1 if off in (0, first[mat][1] // 2) else 2)
            wait_all(peers[key], peer[mat].at[some] if mat == "D" else peer[mat].at[some, :, :, part])
        return [own[mat].at[b, half], peer[mat].at[b, half]]

    def rs_ring(name, axis, n, pos, local, send, recv, index, ssem, dims, finish, times):
        seq, landing_sems = order(n), []

        def cut(ref):
            return ref.at[index] if index else ref

        def wait_both(slot):
            wait_all(landing_sems[slot], recv.at[(slice(None), slot, *index)])

        for i, (far, s) in enumerate(seq):
            prev = seq.index((far, s - 1)) if s > 1 else None
            yield times[i]
            with jax.named_scope(f"{name}_{i}"):
                landing_sems.append(sem())
                if s > 1:
                    wait_both(prev)
                for d in range(2):
                    half = d if far else 1 - d
                    off = n // 2 - s + far
                    off = -off if d and off < n // 2 else off
                    b = (pos + off + n) % n
                    srcs = [cut(r) for r in local(off, b, half)]
                    if s > 1:
                        srcs.append(cut(recv.at[d, prev]))
                    dst = cut(send(d, i, b, half))
                    add_refs(dst, srcs, dims)
                    remote(dst, cut(recv.at[d, i]), ssem, landing_sems[i], ring_ids[axis][d]).start()
        yield times[-1]
        with jax.named_scope(f"{name}_end"):
            wait_both(n - 3)
            wait_both(n - 2)
            for half in range(2):
                finish(half, [cut(recv.at[half, n - 2]), cut(recv.at[1 - half, n - 3])])

    def stage1(mat, axis, part, index, ssem, dims, times):
        p, n = first[mat]

        def cut(ref):
            return ref.at[index] if index else ref

        def finish(half, got):
            add_refs(cut(acc[mat].at[half]), [cut(r) for r in local1(mat, 0, p, half, part)] + got, dims)

        return rs_ring(
            "rs" + mat + axis, axis, n, p, lambda off, b, half: local1(mat, off, b, half, part), lambda d, i, b, half: own[mat].at[b, half],
            r1[mat], index, ssem, dims, finish, times,
        )

    def stage2(mat, axis, pos, index, ssem, dims, finish, times):
        return rs_ring(
            "rs" + mat + axis, axis, N, pos, lambda off, b, half: [acc[mat].at[half, b]], lambda d, i, b, half: s2[mat].at[d, i],
            r2[mat], index, ssem, dims, finish, times,
        )

    def to_z(which, mat, pos, part):
        def finish(half, got):
            here = acc[mat].at[half, pos, tiles(part)]

            total = here[0] + got[0][0].astype(F32) + got[1][0].astype(F32)
            for q in range(NZ):
                one = total[:, LANES * q : LANES * q + LANES]
                accZ[q, half, which, part] = one
                sZ[q, half, which, part] = one.astype(BF16)

        return finish

    ss = {key: group(r) for key, r in (("G1", r1G), ("U1", r1U), ("D1", r1D), ("G2", r2G), ("U2", r2U), ("D2", r2D))}
    ss["Z"], ss["Y"] = group(rZ.at[: NZ - 1]), group(rY.at[: N - 1])

    def across_z(which, part, times):
        got, cut = sem(), tiles(part)
        yield times[0]
        for j in range(1, NZ):
            zz = (z + j) % NZ
            remote(sZ.at[zz, :, which, cut], rZ.at[z, :, which, cut], ss["Z"], got, dev(x, y, zz, c)).start()
        yield times[1]
        with jax.named_scope("rsZ"):
            wait_all(got, rZ.at[: NZ - 1, :, which, cut])
            for half in range(LAYERS):
                total = accZ[z, half, which, part]
                for j in range(1, NZ):
                    total = total + rZ[(z + j) % NZ, half, which, part].astype(F32)
                gsum[half, which, pl.ds(part * ROWS, ROWS)] = total.astype(BF16).astype(F32)

    def rs_pipe(part, tG, tZG, tU, tZU):
        cut1, cut2 = (slice(None), tiles(part)), (tiles(part),)
        long, short = (N, 1), (1,)
        return interleave(
            chain(
                stage1("G", "x", part, cut1, ss["G1"], long, tG[:N]),
                stage2("G", "y", y, cut2, ss["G2"], short, to_z(0, "G", y, part), tG[N:]),
                across_z(0, part, tZG),
            ),
            chain(
                stage1("U", "y", part, cut1, ss["U1"], long, tU[:N]),
                stage2("U", "x", x, cut2, ss["U2"], short, to_z(1, "U", x, part), tU[N:]),
                across_z(1, part, tZU),
            ),
        )

    def finishDx(half, got):
        @pl.loop(0, N)
        def _(i):
            total = accD[half, x, i] + got[0][i].astype(F32) + got[1][i].astype(F32)
            accY[half, i] = total
            sY[i, half] = total.astype(BF16)

    def across_y(times):
        got = sem()
        yield times[0]
        for j in range(1, N):
            yy = (y + j) % N
            remote(sY.at[yy], rY.at[y], ss["Y"], got, dev(x, yy, z, c)).start()
        yield times[1]
        with jax.named_scope("rsY"):
            wait_all(got, rY.at[: N - 1])
            for half in range(LAYERS):
                total = accY[half, y]
                for j in range(1, N):
                    total = total + rY[(y + j) % N, half].astype(F32)
                gsumD[half] = total.astype(BF16).astype(F32)

    mv, mvd = keep(), keep()

    def send_moments():
        yield 11.5
        for one in mloads:
            one.wait()
        for j, ref in enumerate((mG, vG, mU, vU)):
            for l in range(LAYERS):
                for q in range(COLUMN):
                    pk[q, packed_rows(j, l), :] = ref[:, l, LANES * q : LANES * q + LANES]
        for j, ref in enumerate((mD, vD)):
            mvD[j, :, slab(c), :] = ref[:, :, narrow(c)]
        yield 66.5
        ssem, ssemD = group(pk.at[: COLUMN - 1]), group(mvD.at[:, :, :SLAB])
        for j in range(1, COLUMN):
            kk = (k + j) % COLUMN
            remote(pk.at[(kk % 2) * NZ + kk // 2], pkr.at[k], ssem, mv, in_column(kk)).start()
        for j, ref in enumerate((mD, vD)):
            remote(ref.at[:, :, narrow(1 - c)], mvD.at[j, :, slab(c)], ssemD, mvd, partner).start()

    run(interleave(
        chain(
            stage1("D", "z", 0, (), ss["D1"], (N, N), (0, 5, 10, 13, 18, 26, 30, 51)),
            stage2("D", "x", x, (), ss["D2"], (N,), finishDx, (52, 54, 61, 68)),
            across_y((69, 72)),
        ),
        rs_pipe(0, (1, 3, 8, 16, 20, 23, 28, 39), (40, 60), (2, 4, 9, 17, 19, 33, 35, 47), (48, 64)),
        rs_pipe(1, (6, 21, 25, 41, 42, 44, 53, 62), (63, 71), (7, 27, 29, 45, 46, 50, 57, 65), (66, 73)),
        rs_pipe(2, (11, 14, 22, 34, 36, 38, 49, 58), (59, 70), (12, 15, 24, 31, 32, 37, 43, 55), (56, 67)),
        send_moments(),
    ))

    with jax.named_scope("sent"):
        drain()
        counts["reused"] = 0

    with jax.named_scope("norm"):
        total = jnp.zeros((SLAB, LANES), F32)

        def squares(total, g):
            for q in range(g.shape[1] // LANES):
                one = g[:, LANES * q : LANES * q + LANES]
                one = one * one
                total = total + one[:SLAB] + one[SLAB:]
            return total

        for half in range(LAYERS):
            for which in range(2):
                for t in range(TILES):
                    total = squares(total, gsum[half, which, ROWS * t : ROWS * t + ROWS])
            total = squares(total, gsumD[half])
        total = jnp.sum(total, axis=0, keepdims=True)
    rb, rd = keep(), keep()
    gk[:, 2 * LAYERS * TILES :, :] = jnp.zeros((COLUMN, N, LANES), F32)
    for stage, got in enumerate((nr1, nr2)):
        with jax.named_scope(f"norm{stage}"):
            nrm[stage] = total
            here, rsem, ssem = (xy if stage else k), keep(), group(got.at[: COLUMN - 1], keep)
            for j in range(1, COLUMN):
                there = (here + j) % COLUMN
                device = {"dp": there * COLUMN + k} if stage else in_column(there)
                remote(nrm.at[stage], got.at[here], ssem, rsem, device).start()
            if not stage:
                pkr[k] = pk[cb]
                wait_all(mv, pkr.at[: COLUMN - 1])
                for j in range(mvcol.shape[0]):
                    for l in range(LAYERS):
                        for q in range(COLUMN):
                            mvcol[j, l, TILES * q : TILES * q + TILES, :] = pkr[q, packed_rows(j, l), :]
                wait_all(mvd, mvD.at[:, :, :SLAB])
                for one in wloads:
                    one.wait()
            else:
                for q in range(COLUMN):
                    for which in range(2):
                        for l in range(LAYERS):
                            gk[q, packed_rows(which, l), :] = gsum[l, which, TILES * q : TILES * q + TILES, :]
                gs, gsD = group(gk.at[: COLUMN - 1], keep), group(gkD, keep)
                for j in range(1, COLUMN):
                    kk = (k + j) % COLUMN
                    remote(gk.at[kk], gr.at[cb], gs, rb, in_column(kk)).start()
                remote(gsumD.at[:, slab(1 - c)], gkD, gsD, rd, partner).start()
                gr[cb] = gk[k]
            got[here] = nrm[stage]
            wait_all(rsem, got.at[: COLUMN - 1])
            total = got[0]
            for j in range(1, COLUMN):
                total = total + got[j]
    total = jnp.sum(total, axis=1, keepdims=True)
    factor = jnp.minimum(1.0, 0.5 * lax.rsqrt(total / (3 * 2 * 768 * 2048) + 1e-30))

    with jax.named_scope("adamw"):
        for half in range(LAYERS):
            new, _, _ = adamw(wcolD[half].astype(F32), mvD[0, half], mvD[1, half], gsumD[half] * factor)
            oD[half, x, y, z, :, narrow(c)] = new
            for a, out in enumerate((oG, oU)):
                for b in range(TILES):
                    rows = pl.ds(ROWS * b, ROWS)
                    new, _, _ = adamw(
                        wcol[a, half, b].astype(F32), mvcol[2 * a, half, rows], mvcol[2 * a + 1, half, rows], gsum[half, a, rows] * factor
                    )
                    out[half, x, y, b, :, mine] = new

    onward = {mat: (group(peer[mat]), sem()) for mat in peer}

    def ag_ring(name, axis, n, pos, piece, two, ssem, on, times):
        seq, landing_sems = order(n), []

        def pass_on(ref):
            if on:
                remote(ref, ref, *onward[on], partner).start()

        def got(i):
            far, s = seq[i]
            wait_all(landing_sems[i], two)
            for d in range(2):
                pass_on(piece((pos + (s if d else n - s)) % n, d if far else 1 - d))

        for i, (far, s) in enumerate(seq):
            yield times[i]
            with jax.named_scope(f"{name}_{i}"):
                landing_sems.append(sem())
                if s > 1:
                    got(seq.index((far, s - 1)))
                for d in range(2):
                    ref = piece((pos + (s - 1 if d else n - s + 1)) % n, d if far else 1 - d)
                    remote(ref, ref, ssem, landing_sems[i], ring_ids[axis][d]).start()
        for half in range(2):
            pass_on(piece(pos, half))
        for slot in (n - 3, n - 2):
            yield times[slot + 2]
            with jax.named_scope(f"{name}_end{slot}"):
                got(slot)

    others = oD.at[:, :3, 0, :5, :, :NARROW]
    ss = {key: group(r) for key, r in (("G1", r1G), ("U1", r1U), ("D1", r1D), ("G2", r2G), ("U2", r2U), ("D2", others))}
    ss["Z"] = group(rZ.at[: NZ - 1])

    def back_z(out, part, times):
        got = sem()
        yield times[0]
        ref = out.at[:, x, y, tiles(part), :, mine]
        for j in range(1, NZ):
            remote(ref, ref, ss["Z"], got, dev(x, y, (z + j) % NZ, c)).start()
        yield times[1]
        with jax.named_scope("agZ"):
            wait_all(got, rZ.at[: NZ - 1, :, 0, tiles(part)])

    def back_columns(times):
        got = sem()
        yield times[0]
        ref = oD.at[:, x, y, z, :, narrow(c)]
        for j in range(1, COLUMN):
            remote(ref, ref, ss["D2"], got, {"dp": (xy + j) % COLUMN * COLUMN + k}).start()
        yield times[1]
        with jax.named_scope("agXY"):
            wait_all(got, others)

    def ag_pipe(part, tZG, tG, tZU, tU):
        cols, cut, n = wide(c), tiles(part), N + 1
        two1, two2 = r1G.at[:, 0, :, cut], r2G.at[:, 0, cut]
        return interleave(
            chain(
                back_z(oG, part, tZG),
                ag_ring("agGy", "y", N, y, lambda p, half: oG.at[half, x, p, cut, :, cols], two2, ss["G2"], None, tG[:n]),
                ag_ring("agGx", "x", N, x, lambda p, half: oG.at[half, p, :, cut, :, cols], two1, ss["G1"], "G", tG[n:]),
            ),
            chain(
                back_z(oU, part, tZU),
                ag_ring("agUx", "x", N, x, lambda p, half: oU.at[half, p, y, cut, :, cols], two2, ss["U2"], None, tU[:n]),
                ag_ring("agUy", "y", N, y, lambda p, half: oU.at[half, :, p, cut, :, cols], two1, ss["U1"], "U", tU[n:]),
            ),
        )

    def new_moments():
        yield 7
        with jax.named_scope("moments"):
            wait_all(rb, gr.at[: COLUMN - 1])
            wait_all(rd, gkD)
            for which, (m, v, om, ov) in enumerate(((mG, vG, omG, ovG), (mU, vU, omU, ovU))):
                for l in range(LAYERS):
                    for q in range(COLUMN):
                        cols = slice(LANES * q, LANES * q + LANES)
                        om[:, l, cols], ov[:, l, cols] = moments(m[:, l, cols], v[:, l, cols], gr[q, packed_rows(which, l), :] * factor)
            for cols, g in ((narrow(c), gsumD[:, slab(c), :]), (narrow(1 - c), gkD[...])):
                omD[:, :, cols], ovD[:, :, cols] = moments(mD[:, :, cols], vD[:, :, cols], g * factor)

    run(interleave(
        chain(
            back_columns((5, 18)),
            ag_ring("agDz", "z", NZ, z, lambda p, half: oD.at[half, :, :, p, :, narrow(c)], r1D.at[:, 0], ss["D1"], "D", (19, 20, 47, 54, 61, 67, 73, 78, 81)),
        ),
        ag_pipe(0, (0, 8), (9, 10, 17, 21, 31, 32, 33, 52, 55, 68), (1, 11), (12, 13, 25, 26, 39, 40, 41, 53, 58, 72)),
        ag_pipe(1, (4, 27), (28, 29, 43, 46, 59, 60, 65, 74, 79, 82), (6, 35), (36, 37, 56, 57, 69, 70, 71, 77, 80, 83)),
        ag_pipe(2, (3, 22), (23, 24, 38, 42, 48, 49, 50, 62, 64, 76), (2, 14), (15, 16, 30, 34, 44, 45, 51, 63, 66, 75)),
        new_moments(),
    ))

    with jax.named_scope("drain"):
        for mat in peer:
            wait_all(onward[mat][1], peer[mat])
        drain()
    assert (counts["kept"], max(used)) == (KEPT, REUSED), (counts["kept"], max(used))


def store(*refs):
    *refs, sem = refs
    half = len(refs) // 2
    pairs = list(zip(refs[:half], refs[half:], strict=True))
    for j, (i, o) in enumerate(pairs):
        if len(o.shape) > TILES:
            for l in range(LAYERS):
                for p in range(N):
                    pltpu.make_async_copy(i.at[l, p], o.at[l, p], sem.at[j]).start()
        else:
            pltpu.make_async_copy(i, o, sem.at[j]).start()
    for j, (i, o) in enumerate(pairs):
        pltpu.make_async_copy(i, o, sem.at[j]).wait()


def fused(*arrays):
    g, w, m, v = (arrays[i : i + 3] for i in (0, 3, 6, 9))
    big, low = (N, TILES, ROWS, WIDE), (N, N, ROWS, NARROW)
    view = (LAYERS, N, N, TILES, ROWS, 2 * WIDE)
    views = [view, view, (LAYERS, N, N, NZ, ROWS, 2 * NARROW)]
    g = [one.reshape(s) for one, s in zip(g, views, strict=True)]
    w = [one.reshape(s) for one, s in zip(w, views, strict=True)]
    m, v = ([jnp.swapaxes(one, 0, 1) if one.shape[1] == TILES else one for one in t] for t in (m, v))
    vm, hbm, D = pl.BlockSpec(memory_space=pltpu.VMEM), pl.BlockSpec(memory_space=pl.ANY), pltpu.SemaphoreType.DMA

    def V(dtype, *shape):
        return pltpu.VMEM(shape, dtype)

    tile, packed, rows48 = (TILES, ROWS, LANES), (COLUMN, N * LAYERS * TILES, LANES), (TILES * ROWS, LANES)
    mine = [V(F32, *one.shape) for one in (m[0], m[1], v[0], v[1], m[2], v[2])]
    scratch = [
        *[V(BF16, N, LAYERS, *big)] * 4, *[V(BF16, NZ, LAYERS, *low)] * 2,
        *[V(F32, LAYERS, *big)] * 2, V(F32, LAYERS, *low), V(F32, NZ, LAYERS, 2, *tile), V(F32, LAYERS, *low[1:]),
        *[V(BF16, 2, N - 1, *big)] * 2, V(BF16, 2, NZ - 1, *low),
        *[V(BF16, 2, N - 1, *big[1:])] * 4, *[V(BF16, 2, N - 1, *low[1:])] * 2,
        *[V(BF16, N, LAYERS, *low[2:])] * 2, *[V(BF16, NZ, LAYERS, 2, *tile)] * 2,
        V(F32, LAYERS, 2, *rows48), V(F32, LAYERS, *low[2:]), V(BF16, 2, LAYERS, *tile), V(BF16, LAYERS, *low[2:]),
        V(F32, N, LAYERS, *rows48), V(F32, 2, LAYERS, *low[2:]), *[V(F32, *packed)] * 2,
        *[V(F32, COLUMN, ROWS, LANES)] * 2, V(F32, LAYERS, SLAB, NARROW),
        V(F32, 2, 1, LANES), *[V(F32, COLUMN, 1, LANES)] * 2, *mine, D((KEPT,)), D((REUSED,)),
    ]
    passed = pl.pallas_call(
        kernel,
        out_shape=[V(BF16, *s) for s in views] + [V(F32, *one.shape) for one in (*m, *v)],
        in_specs=[hbm] * 12,
        out_specs=[vm] * 9,
        scratch_shapes=scratch,
        compiler_params=pltpu.CompilerParams(collective_id=0, has_side_effects=True, vmem_limit_bytes=VMEM_LIMIT),
        name="step",
    )(*g, *w, *m, *v)
    outs = pl.pallas_call(
        store,
        out_shape=[jax.ShapeDtypeStruct(s, BF16) for s in views] + [jax.ShapeDtypeStruct(one.shape, F32) for one in (*m, *v)],
        in_specs=[vm] * 9,
        out_specs=[hbm] * 9,
        scratch_shapes=[D((9,))],
        compiler_params=pltpu.CompilerParams(vmem_limit_bytes=2**20),
        name="store",
    )(*passed)
    outs = [jnp.swapaxes(o, 0, 1) if o.shape[0] == TILES else o for o in outs]
    return tuple(o.reshape(one.shape) for o, one in zip(outs, (*arrays[3:6], *arrays[6:]), strict=True))


def solution(mesh):
    all_of, cut = P(None, None, None), P(None, "dp", None)
    return jax.shard_map(
        fused,
        mesh=mesh,
        in_specs=(P(("rep", "dp"), None, None, None),) * 3 + (all_of,) * 3 + (cut,) * 6,
        out_specs=(P("rep", None, None),) * 3 + (P("rep", "dp", None),) * 6,
        check_vma=False,
    )
```
